512 devices in a mesh: dp: 8 (over z), expert: 64 (over y, x, core).
Axes of the slice: x: 4, y: 8, z: 8, core: 2. Of those that a mesh axis runs over, the one named last changes fastest.
Arguments:
- expert_out: bfloat16 [8, 128, 64, 2, 7168], P('dp', 'expert'), may hold values from -6 to 6
- expert_ids: int32 [4096, 8], P(('dp', 'expert')), may hold values from 0 to 127, all different within a row; in each aligned block of 8 rows (0 to 7, 8 to 15, ...) at most 2 rows name the same one
- gate_weight: float32 [4096, 8], P(('dp', 'expert')), may hold values from 0.05 to 1
Outputs:
- combined: bfloat16 [4096, 7168], P(('dp', 'expert'))
- expert_counts: int32 [128], P('expert')
- expert_rms: float32 [128], P('expert')
The draws below stay inside these ranges and needn't reach their ends.
Inputs may be any that keep to these rules, and one draw needn't show every extreme that they name: `expert_ids`: in each aligned block of 8 tokens no expert is named by more than 2 rows, and a token names 8 different experts; every expert is named by some token.
All inputs are finite; a program needn't handle non-finite values.
Results may differ from the reference program's by a relative error of at most 0.008.
Values may be sent and summed in bfloat16 or wider, within the bound.
A program may use at most 64 MiB of HBM per device.

```python
import math
import jax
import jax.numpy as jnp
import numpy as np
from jax import lax

D = 7168
EXPERTS = 128
TOP = 8
TOK_DEV = 8
CAP = 2
TOKENS = 4096
N_DP = 8
N_EXPERT = 64


def steps_of(stream_key, dims, pieces, low, high):
    gain, own = 1.0, jax.random.fold_in(stream_key, 6)
    for axis_at, blocks in pieces:
        steps = jnp.exp(jax.random.uniform(jax.random.fold_in(own, axis_at), (blocks,), jnp.float32, low / len(pieces), high / len(pieces)))
        gain = gain * jnp.repeat(steps, dims[axis_at] // blocks).reshape([-1 if axis == axis_at else 1 for axis in range(len(dims))])
    return gain


def shared_out(stream_key, own, number, rows, amount, top, bound, slope):
    sequence = jax.random.permutation(stream_key, amount)
    crowded, common = load_shares(amount, rows * top, bound, slope, True), load_shares(amount, rows * top, bound, slope, False)
    places = jnp.arange(amount)

    def named(tallies, offset_by):
        used = int((tallies > 0).sum())
        fixed = max(1, used // 4)
        moved = fixed + (places - fixed + offset_by * (used - fixed)) % max(1, amount - fixed)
        return jnp.zeros((amount,), jnp.int32).at[sequence[jnp.where(places < fixed, places, moved)]].set(jnp.asarray(tallies, jnp.int32))

    tallies = jnp.where(number % 4 == 0, named(crowded, number // 4), named(common, number - number // 4 - 1))
    mixed = jax.random.permutation(jax.random.fold_in(own, 3), amount)
    giver, sink = mixed[0:amount // 2 * 2:2], mixed[1:amount // 2 * 2:2]
    margin = jnp.minimum(tallies[giver] - 1, bound - tallies[sink]) // 2
    margin = jnp.where((giver == sequence[0]) | (sink == sequence[0]) | (tallies[sink] == 0), 0, jnp.maximum(margin, 0))
    moved = jax.random.randint(jax.random.fold_in(own, 4), (amount // 2,), 0, 1 << 20) % (margin + 1)
    tallies = tallies.at[giver].add(-moved).at[sink].add(moved)
    members = jnp.searchsorted(jnp.cumsum(tallies), jnp.arange(rows * top), side="right").astype(jnp.int32)
    listing = members.reshape(top, rows).T
    listing = listing[jax.random.permutation(jax.random.fold_in(own, 1), rows)]
    offset_by = jax.random.randint(jax.random.fold_in(own, 2), (rows, 1), 0, top)
    return jnp.take_along_axis(listing, (jnp.arange(top)[None, :] + offset_by) % top, axis=1)


def load_shares(amount, total, most, slope, full):
    weights = [(1 << 20) // math.isqrt(grade ** slope) + 1 for grade in range(1, amount + 1)]
    largest = most if full else min(most, max(-(-total // amount), total * weights[0] // sum(weights)))
    least = 1 if total - largest >= amount - 1 else 0
    given, spare = [largest] + [least] * (amount - 1), total - largest - least * (amount - 1)
    while spare > 0:
        movable = [i for i in range(1, amount) if given[i] < largest] or [i for i in range(1, amount) if given[i] < most]
        whole, budget = sum([weights[i] for i in movable]), spare
        for i in movable:
            more = min(most - given[i], max(1, budget * weights[i] // whole), spare)
            given[i] = given[i] + more
            spare = spare - more
    return np.array(given)


def scatter_about(own_key, shape, spread, reach, pieces=(), kind=jnp.bfloat16):
    factor_of = steps_of(own_key, shape, pieces, -0.22, 0.18) if pieces else 1.0
    values = jax.random.normal(own_key, shape, jnp.float32) * spread * factor_of
    return jnp.minimum(jnp.maximum(values, -reach), reach).astype(kind)


def setup_inputs(seed: int = 0) -> dict:
    splits = jax.random.split(jax.random.key(seed), 4)
    expert_out = scatter_about(splits[0], (N_DP, EXPERTS, N_EXPERT, CAP, D), 1.0, 6.0, ((0, 8), (1, 64)))
    expert_ids_keys = jax.random.split(jax.random.fold_in(splits[1], 1), TOKENS // TOK_DEV)
    expert_ids_turns = jax.random.permutation(jax.random.fold_in(splits[1], 3), TOKENS // TOK_DEV)
    expert_ids = jax.vmap(lambda own, number: shared_out(jax.random.fold_in(splits[1], 2), own, number, TOK_DEV, EXPERTS, TOP, CAP, 2))(expert_ids_keys, expert_ids_turns).reshape((TOKENS, TOP))
    gate_weight = jnp.clip(0.05 + 0.95 * jax.random.uniform(splits[2], (TOKENS, TOP), jnp.float32) ** steps_of(splits[2], (TOKENS, TOP), ((0, 512),), -0.2, 0.2), 0.05, 1.0)
    return {"expert_out": expert_out, "expert_ids": expert_ids, "gate_weight": gate_weight}


epsilon = 1e-06

def slot_index_of(block_ids):
    flat = block_ids.reshape(-1).astype(jnp.int32)
    total_rows = flat.shape[0]
    one_hot = (flat[:, None] == jnp.arange(EXPERTS, dtype=jnp.int32)[None, :]).astype(jnp.float32)
    earlier = (jnp.arange(total_rows, dtype=jnp.int32)[:, None] > jnp.arange(total_rows, dtype=jnp.int32)[None, :]).astype(jnp.float32)
    before = jnp.dot(earlier, one_hot, precision=lax.Precision.HIGHEST)
    position = lax.optimization_barrier(jnp.sum(before * one_hot, axis=1)).astype(jnp.int32)
    return flat * CAP + position

def holder_combine(picked, ids, gates, per_holder):
    holder = ids // per_holder
    same = (holder[:, :, None] == holder[:, None, :]).astype(jnp.float32)
    weights = same * gates[:, None, :].astype(jnp.float32)
    partial_value = jnp.einsum('tkj,tjd->tkd', weights, picked.astype(jnp.float32), precision=lax.Precision.HIGHEST)
    partial_value = partial_value.astype(jnp.bfloat16).astype(jnp.float32)
    lower = (jnp.arange(TOP, dtype=jnp.int32)[:, None] > jnp.arange(TOP, dtype=jnp.int32)[None, :]).astype(jnp.float32)
    repeats = lax.optimization_barrier(jnp.sum(same * lower[None, :, :], axis=2))
    leading = (repeats < 0.5).astype(jnp.float32)
    return lax.optimization_barrier(jnp.sum(leading[:, :, None] * partial_value, axis=1)).astype(jnp.bfloat16)

def reference(expert_out, expert_ids, gate_weight):
    blocks = N_DP * N_EXPERT
    per_holder = EXPERTS // N_EXPERT
    id_blocks = expert_ids.reshape(blocks, TOK_DEV, TOP)
    gate_blocks = gate_weight.reshape(blocks, TOK_DEV, TOP)

    def one_block(block_id):
        group = block_id // N_EXPERT
        source = block_id % N_EXPERT
        slab = lax.dynamic_index_in_dim(expert_out, group, 0, keepdims=False)
        slab = lax.dynamic_index_in_dim(slab, source, 1, keepdims=False)
        received = slab.reshape(EXPERTS * CAP, D)
        block_ids = lax.dynamic_index_in_dim(id_blocks, block_id, 0, keepdims=False)
        gates = lax.dynamic_index_in_dim(gate_blocks, block_id, 0, keepdims=False)
        slot_index = slot_index_of(block_ids)
        picked = jnp.take(received, slot_index, axis=0).reshape(TOK_DEV, TOP, D)
        mixed_block = holder_combine(picked, block_ids, gates, per_holder)
        occupied = lax.optimization_barrier(jnp.sum((slot_index[:, None] == jnp.arange(EXPERTS * CAP, dtype=jnp.int32)[None, :]).astype(jnp.float32), axis=0))
        squares = lax.optimization_barrier(jnp.sum(jnp.square(received.astype(jnp.float32)), axis=1))
        sum_squares = lax.optimization_barrier(jnp.sum((occupied * squares).reshape(EXPERTS, CAP), axis=1))
        count_part = lax.optimization_barrier(jnp.sum(occupied.reshape(EXPERTS, CAP), axis=1))
        return (mixed_block, sum_squares, count_part)
    mixed_blocks, sums, counts = lax.map(one_block, jnp.arange(blocks, dtype=jnp.int32))
    combined = mixed_blocks.reshape(TOKENS, D)
    total_counts = lax.optimization_barrier(jnp.sum(counts, axis=0))
    total_squares = lax.optimization_barrier(jnp.sum(sums, axis=0))
    expert_rms = jnp.sqrt(total_squares / (total_counts * D) + epsilon)
    return (combined, total_counts.astype(jnp.int32), expert_rms)
```

```python
import jax
import jax.numpy as jnp
from jax import lax
from jax.experimental import pallas as pl
from jax.experimental.pallas import tpu as pltpu
from jax.sharding import PartitionSpec as P

TOP = 8
NX, NY, NZ = 4, 8, 8
LANES = 128
ROWS = 16
TOK = 64
EPS = 1e-06
MESH = pl.DeviceIdType.MESH
BF16, F32 = jnp.bfloat16, jnp.float32


def wrap(value, size):
    return lax.rem(value + size, size)


def shift_rows(v, by, row):
    return jnp.where(row >= by, pltpu.roll(v, by, 0), 0.0)


def kernel(
    chunks, x_ref, meta_ref, out_ref, stat_ref,
    raw, far_a, far_b, near_a, near_b, comb_r, comb_l, comb_a, comb_b, summed, y_in,
    meta, weights, stat, stat_pair, stat_z,
    loc_sem, swap_sem, far_sem, near_sem, comb_sem, y_sem, meta_x_sem, meta_y_sem, pair_sem, z_sem,
):
    z = lax.axis_index("dp")
    d = lax.axis_index("expert")
    c = lax.rem(d, 2)
    x = lax.rem(lax.div(d, 2), NX)
    y = lax.div(d, 2 * NX)
    xr, xl, xf = wrap(x + 1, NX), wrap(x + NX - 1, NX), wrap(x + 2, NX)

    def at(yy, xx, cc):
        return (yy * NX + xx) * 2 + cc

    partner, right, left = at(y, x, 1 - c), at(y, xr, c), at(y, xl, c)
    x_peers = [at(y, wrap(x + k, NX), c) for k in range(1, NX)]
    y_peers = [at(wrap(y + k, NY), x, c) for k in range(1, NY)]
    z_peers = [wrap(z + k, NZ) for k in range(1, NZ)]

    def send(src, dst, sems, index, device):
        copy = pltpu.make_async_remote_copy(
            src_ref=src, dst_ref=dst, send_sem=sems.at[(0, *index)], recv_sem=sems.at[(1, *index)],
            device_id=device, device_id_type=MESH,
        )
        copy.start()
        return copy

    own = [
        pltpu.make_async_copy(
            x_ref.at[:, :, :, c, pl.ds(ROWS * q, ROWS), :], raw.at[q, pl.ds(2 * c, 2)], loc_sem.at[q]
        )
        for q in range(chunks)
    ]
    for copy in own:
        copy.start()
    meta[y, x] = meta_ref[...]

    barrier = pltpu.get_barrier_semaphore()
    greeted = [(z, partner)] + [(z, p) for p in x_peers + y_peers] + [(p, d) for p in z_peers]
    for device in greeted:
        pl.semaphore_signal(barrier, inc=1, device_id=device, device_id_type=MESH)
    pl.semaphore_wait(barrier, len(greeted))

    sent = []
    meta_x = [
        send(meta_ref, meta.at[y, x], meta_x_sem, (k,), (z, p)) for k, p in enumerate(x_peers)
    ]
    swap = [
        send(
            x_ref.at[:, :, :, 1 - c, pl.ds(ROWS * q, ROWS), :], raw.at[q, pl.ds(2 * c, 2)],
            swap_sem, (q,), (z, partner),
        )
        for q in range(chunks)
    ]
    sent += meta_x + swap
    far, near, comb, to_y = {}, {}, {}, {}

    def send_far(q):
        own[q].wait()
        swap[q].wait_recv()
        far[q] = [
            send(raw.at[q, :, pl.ds(0, 4), xf], far_a.at[q], far_sem, (0, q), (z, right)),
            send(raw.at[q, :, pl.ds(4, 4), xf], far_b.at[q], far_sem, (1, q), (z, left)),
        ]
        sent.extend(far[q])

    def send_near(q):
        near[q] = [
            send(raw.at[q, :, pl.ds(4, 4), xr], near_b.at[q], near_sem, (0, q), (z, right)),
            send(raw.at[q, :, pl.ds(0, 4), xl], near_a.at[q], near_sem, (1, q), (z, left)),
        ]
        sent.extend(near[q])

    def mixed(index, q, yy, column, other):
        rows = jnp.concatenate(
            [raw[q, :, yy, column].reshape(4 * ROWS, LANES), other.reshape(4 * ROWS, LANES)], axis=0
        )
        return jnp.dot(weights[index], rows, preferred_element_type=F32)

    def send_comb(q):
        for copy in far[q]:
            copy.wait_recv()
        for h in range(4):
            comb_r[q, h] = mixed(h, q, h, xr, far_a[q, :, h]).astype(BF16)
        for h in range(4):
            comb_l[q, h] = mixed(4 + h, q, 4 + h, xl, far_b[q, :, h]).astype(BF16)
        comb[q] = [
            send(comb_r.at[q], comb_a.at[q], comb_sem, (0, q), (z, right)),
            send(comb_l.at[q], comb_b.at[q], comb_sem, (1, q), (z, left)),
        ]
        sent.extend(comb[q])

    def send_y(q):
        for copy in near[q] + comb[q]:
            copy.wait_recv()
        for h in range(4):
            total = mixed(8 + h, q, h, x, near_a[q, :, h]) + comb_a[q, h].astype(F32)
            summed[q, h] = total.astype(BF16)
        for h in range(4):
            total = mixed(12 + h, q, 4 + h, x, near_b[q, :, h]) + comb_b[q, h].astype(F32)
            summed[q, 4 + h] = total.astype(BF16)
        to_y[q] = [
            send(summed.at[q, wrap(y + k, NY)], y_in.at[q, k - 1], y_sem, (q, k - 1), (z, y_peers[k - 1]))
            for k in (4, 3, 5, 2, 6, 1, 7)
        ]
        sent.extend(to_y[q])

    def finish(q):
        for copy in to_y[q]:
            copy.wait_recv()
        total = summed[q, y].astype(F32)
        for k in range(NY - 1):
            total = total + y_in[q, k].astype(F32)
        out_ref[q] = total.astype(BF16)

    lane = lax.broadcasted_iota(jnp.int32, (8, LANES), 1)
    row = lax.broadcasted_iota(jnp.int32, (8, LANES), 0)

    def build(index, yy, column, other):
        chip = jnp.where(lane < LANES // 2, y * NX + x, y * NX + other)
        expert = (chip * 4 + lax.rem(lax.div(lane, ROWS), 4)).astype(F32)
        slot = lax.rem(lane, 2).astype(F32)
        tile = lax.rem(lax.div(lane, 2), 8)
        block = meta[yy, column]
        names = jnp.zeros((8, LANES), F32)
        gates = jnp.zeros((8, LANES), F32)
        for k in range(TOP):
            hit = block[:, k : k + 1] == expert
            names = names + jnp.where(hit, 1.0, 0.0)
            gates = gates + jnp.where(hit, block[:, TOP + k : TOP + k + 1], 0.0)
        earlier = shift_rows(names, 1, row)
        for by in (1, 2, 4):
            earlier = earlier + shift_rows(earlier, by, row)
        gates = jnp.where(earlier == slot, gates, 0.0)
        spread = jnp.concatenate([jnp.where(tile == j, gates, 0.0) for j in range(8)], axis=0)
        weights[index] = spread.astype(BF16)

    def count_and_square():
        expert = ((y * NX + x) * 4 + lane).astype(F32)
        odd = lax.rem(row, 2).astype(F32)

        def step(b, carry):
            yy, xx = lax.div(b, NX), lax.rem(b, NX)
            block = meta[yy, xx]
            names = jnp.zeros((8, LANES), F32)
            for k in range(TOP):
                names = names + jnp.where(block[:, k : k + 1] == expert, 1.0, 0.0)
            named = jnp.broadcast_to(jnp.sum(names, axis=0, keepdims=True), (8, LANES))
            squares, counts = list(carry[:4]), list(carry[4:])
            for e in range(4):
                much = jnp.broadcast_to(named[:, e : e + 1], (8, LANES))
                total = jnp.zeros((8, LANES), F32)
                for q in range(chunks):
                    v = raw[q, e, yy, xx].astype(F32)
                    v = v * v
                    total = total + (v[:8] + v[8:])
                squares[e] = squares[e] + jnp.where(odd < much, total, 0.0)
                counts[e] = counts[e] + much
            return (*squares, *counts)

        parts = lax.fori_loop(0, NX * NY, step, tuple(jnp.zeros((8, LANES), F32) for _ in range(8)))
        tile = jnp.zeros((8, LANES), F32)
        for e in range(4):
            total = jnp.sum(jnp.sum(parts[e], axis=0, keepdims=True), axis=1, keepdims=True)
            tile = jnp.where(row == e, jnp.broadcast_to(total, (8, LANES)), tile)
            tile = jnp.where(row == 4 + e, parts[4 + e], tile)
        stat[0] = tile

    send_far(0)
    send_far(1)
    send_near(0)
    for copy in meta_x:
        copy.wait_recv()
    meta_y = [
        send(meta.at[y], meta.at[y], meta_y_sem, (k,), (z, p)) for k, p in enumerate(y_peers)
    ]
    sent += meta_y
    send_far(2)
    send_near(1)
    for copy in meta_y:
        copy.wait_recv()
    for h in range(4):
        build(h, h, xr, xl)
        build(4 + h, 4 + h, xl, xr)
    ready = False
    pair, to_z = None, None
    for q in range(chunks):
        send_comb(q)
        if q + 3 < chunks:
            send_far(q + 3)
        if q + 2 < chunks:
            send_near(q + 2)
        if not ready:
            for h in range(4):
                build(8 + h, h, x, xr)
                build(12 + h, 4 + h, x, xl)
            ready = True
        if q >= 1:
            send_y(q - 1)
        if q == chunks - 3:
            count_and_square()
            pair = send(stat.at[0], stat_pair, pair_sem, (), (z, partner))
            sent.append(pair)
        if q == chunks - 2:
            pair.wait_recv()
            stat[1] = stat[0] + stat_pair[...]
        if q == chunks - 1:
            to_z = [
                send(stat.at[1], stat_z.at[k], z_sem, (k,), (p, d)) for k, p in enumerate(z_peers)
            ]
            sent += to_z
        if q >= 3:
            finish(q - 3)
    send_y(chunks - 1)
    finish(chunks - 3)
    for copy in to_z:
        copy.wait_recv()
    total = stat[1]
    for k in range(NZ - 1):
        total = total + stat_z[k]
    squares = jnp.where(c == 0, total[0:2], total[2:4])
    counts = jnp.where(c == 0, total[4:6], total[6:8])
    stat_ref[0:2] = jnp.sqrt(squares / (counts * float(chunks * 8 * LANES)) + EPS)
    stat_ref[2:4] = counts
    stat_ref[4:8] = jnp.zeros((4, LANES), F32)
    finish(chunks - 2)
    finish(chunks - 1)
    for copy in sent:
        copy.wait_send()


def body(expert_out, expert_ids, gate_weight):
    width = expert_out.shape[4]
    tiles = width // LANES
    chunks = tiles // 8
    view = expert_out.reshape(2, NY, NX, 2, 2, tiles, LANES)
    view = view.transpose(0, 1, 2, 3, 5, 4, 6).reshape(2, NY, NX, 2, tiles * 2, LANES)
    meta = jnp.concatenate([expert_ids.astype(F32), gate_weight], axis=1)
    meta = jnp.pad(meta, ((0, 0), (0, LANES - 2 * TOP)))

    def vmem(*shape):
        return pltpu.VMEM(shape, BF16)

    def dma(*shape):
        return pltpu.SemaphoreType.DMA(shape)

    half = (chunks, 4, 4, ROWS, LANES)
    done = (chunks, 4, TOK, LANES)
    out, stats = pl.pallas_call(
        lambda *refs: kernel(chunks, *refs),
        out_shape=(
            jax.ShapeDtypeStruct((chunks, TOK, LANES), BF16),
            jax.ShapeDtypeStruct((8, LANES), F32),
        ),
        in_specs=[pl.BlockSpec(memory_space=pltpu.HBM), pl.BlockSpec(memory_space=pltpu.VMEM)],
        out_specs=(pl.BlockSpec(memory_space=pltpu.VMEM), pl.BlockSpec(memory_space=pltpu.VMEM)),
        scratch_shapes=[
            vmem(chunks, 4, NY, NX, ROWS, LANES),
            vmem(*half), vmem(*half), vmem(*half), vmem(*half),
            vmem(*done), vmem(*done), vmem(*done), vmem(*done),
            vmem(chunks, NY, TOK, LANES), vmem(chunks, NY - 1, TOK, LANES),
            pltpu.VMEM((NY, NX, 8, LANES), F32), vmem(16, TOK, LANES),
            pltpu.VMEM((2, 8, LANES), F32), pltpu.VMEM((8, LANES), F32),
            pltpu.VMEM((NZ - 1, 8, LANES), F32),
            dma(chunks), dma(2, chunks), dma(2, 2, chunks), dma(2, 2, chunks), dma(2, 2, chunks),
            dma(2, chunks, NY - 1), dma(2, NX - 1), dma(2, NY - 1), dma(2), dma(2, NZ - 1),
        ],
        compiler_params=pltpu.CompilerParams(
            collective_id=0, has_side_effects=True
        ),
    )(view, meta)
    combined = out.reshape(tiles, TOP, LANES).transpose(1, 0, 2).reshape(TOP, width)
    return combined, stats[2:4, 0].astype(jnp.int32), stats[0:2, 0]


def solution(mesh):
    return jax.shard_map(
        body,
        mesh=mesh,
        in_specs=(
            P("dp", "expert", None, None, None),
            P(("dp", "expert"), None),
            P(("dp", "expert"), None),
        ),
        out_specs=(P(("dp", "expert"), None), P("expert"), P("expert")),
        check_vma=False,
    )
```

```python
import jax
import jax.numpy as jnp
from jax import lax
from jax.experimental import pallas as pl
from jax.experimental.pallas import tpu as pltpu
from jax.sharding import PartitionSpec as P

TOP = 8
NX, NY, NZ = 4, 8, 8
LANES = 128
ROWS = 16
TOK = 64
EPS = 1e-06
MESH = pl.DeviceIdType.MESH
BF16, F32 = jnp.bfloat16, jnp.float32


def wrap(value, size):
    return lax.rem(value + size, size)


def shift_rows(v, by, row):
    return jnp.where(row >= by, pltpu.roll(v, by, 0), 0.0)


def kernel(
    chunks, x_ref, ids_ref, gates_ref, out_ref, stat_ref,
    raw, far_a, far_b, near_a, near_b, comb_r, comb_l, comb_a, comb_b, summed, y_in, y_raw, x_sum, x_in,
    meta, weights, squares_of, stat, stat_pair, stat_z,
    loc_sem, swap_sem, far_sem, near_sem, comb_sem, y_sem, y_raw_sem, x_sum_sem, meta_sem, pair_sem, z_sem,
):
    z = lax.axis_index("dp")
    d = lax.axis_index("expert")
    c = lax.rem(d, 2)
    x = lax.rem(lax.div(d, 2), NX)
    y = lax.div(d, 2 * NX)
    xr, xl, xf = wrap(x + 1, NX), wrap(x + NX - 1, NX), wrap(x + 2, NX)

    def at(yy, xx, cc):
        return (yy * NX + xx) * 2 + cc

    last = chunks - 1
    partner, right, left = at(y, x, 1 - c), at(y, xr, c), at(y, xl, c)
    plane = [(i, j) for j in range(NX) for i in range(NY) if (i, j) != (0, 0)]
    peers = [at(wrap(y + i, NY), wrap(x + j, NX), c) for i, j in plane]
    x_peers = [at(y, wrap(x + k, NX), c) for k in range(1, NX)]
    y_peers = [at(wrap(y + k, NY), x, c) for k in range(1, NY)]
    z_peers = [wrap(z + k, NZ) for k in range(1, NZ)]

    def send(src, dst, sems, index, device):
        copy = pltpu.make_async_remote_copy(
            src_ref=src, dst_ref=dst, send_sem=sems.at[(0, *index)], recv_sem=sems.at[(1, *index)],
            device_id=device, device_id_type=MESH,
        )
        copy.start()
        return copy

    own = [
        pltpu.make_async_copy(
            x_ref.at[:, :, :, c, pl.ds(ROWS * q, ROWS), :], raw.at[q, pl.ds(2 * c, 2)], loc_sem.at[q]
        )
        for q in range(chunks)
    ]
    for copy in own:
        copy.start()
    meta[y, x] = jnp.zeros((8, LANES), F32)
    meta[y, x, :, 0:TOP] = ids_ref[...].astype(F32)
    meta[y, x, :, TOP : 2 * TOP] = gates_ref[...]

    barrier = pltpu.get_barrier_semaphore()
    greeted = [(z, partner)] + [(z, p) for p in peers] + [(p, d) for p in z_peers]
    for device in greeted:
        pl.semaphore_signal(barrier, inc=1, device_id=device, device_id_type=MESH)
    pl.semaphore_wait(barrier, len(greeted))

    sent = []
    meta_all = [
        send(meta.at[y, x], meta.at[y, x], meta_sem, (k,), (z, p)) for k, p in enumerate(peers)
    ]
    swap = {
        q: send(
            x_ref.at[:, :, :, 1 - c, pl.ds(ROWS * q, ROWS), :], raw.at[q, pl.ds(2 * c, 2)],
            swap_sem, (q,), (z, partner),
        )
        for q in (0, last, *range(1, last))
    }
    sent += meta_all + list(swap.values())
    far, near, comb, to_y = {}, {}, {}, {}

    def send_far(q):
        if q < 3:
            own[q].wait()
            swap[q].wait_recv()
        far[q] = [
            send(raw.at[q, :, pl.ds(0, 4), xf], far_a.at[q], far_sem, (0, q), (z, right)),
            send(raw.at[q, :, pl.ds(4, 4), xf], far_b.at[q], far_sem, (1, q), (z, left)),
        ]
        sent.extend(far[q])

    def send_near(q):
        near[q] = [
            send(raw.at[q, :, pl.ds(4, 4), xr], near_b.at[q], near_sem, (0, q), (z, right)),
            send(raw.at[q, :, pl.ds(0, 4), xl], near_a.at[q], near_sem, (1, q), (z, left)),
        ]
        sent.extend(near[q])

    def mixed(index, q, yy, column, other):
        rows = jnp.concatenate(
            [raw[q, :, yy, column].reshape(4 * ROWS, LANES), other.reshape(4 * ROWS, LANES)], axis=0
        )
        return jnp.dot(weights[index], rows, preferred_element_type=F32)

    def send_comb(q):
        for copy in far[q]:
            copy.wait_recv()
        for h in range(4):
            comb_r[q, h] = mixed(h, q, h, xr, far_a[q, :, h]).astype(BF16)
        for h in range(4):
            comb_l[q, h] = mixed(4 + h, q, 4 + h, xl, far_b[q, :, h]).astype(BF16)
        comb[q] = [
            send(comb_r.at[q], comb_a.at[q], comb_sem, (0, q), (z, right)),
            send(comb_l.at[q], comb_b.at[q], comb_sem, (1, q), (z, left)),
        ]
        sent.extend(comb[q])

    def send_y(q):
        for copy in near[q] + comb[q]:
            copy.wait_recv()
        for h in range(4):
            total = mixed(8 + h, q, h, x, near_a[q, :, h]) + comb_a[q, h].astype(F32)
            summed[q, h] = total.astype(BF16)
        for h in range(4):
            total = mixed(12 + h, q, 4 + h, x, near_b[q, :, h]) + comb_b[q, h].astype(F32)
            summed[q, 4 + h] = total.astype(BF16)
        to_y[q] = [
            send(summed.at[q, wrap(y + k, NY)], y_in.at[q, k - 1], y_sem, (q, k - 1), (z, y_peers[k - 1]))
            for k in (4, 3, 5, 2, 6, 1, 7)
        ]
        sent.extend(to_y[q])

    def send_y_raw():
        own[last].wait()
        swap[last].wait_recv()
        copies = {
            k: send(
                raw.at[last, :, wrap(y + k, NY)], y_raw.at[k - 1], y_raw_sem, (k - 1,), (z, y_peers[k - 1])
            )
            for k in (4, 3, 5, 2, 6, 1, 7)
        }
        sent.extend(copies.values())
        return copies

    def send_x_sum():
        for copy in y_raw_copies.values():
            copy.wait_recv()
        for xx in range(NX):
            total = jnp.zeros((TOK, LANES), F32)
            for pair_of in range(NY // 2):
                first = raw[last, :, y, xx] if pair_of == 0 else y_raw[2 * pair_of - 1, :, xx]
                second = y_raw[2 * pair_of, :, xx]
                rows = jnp.concatenate(
                    [first.reshape(4 * ROWS, LANES), second.reshape(4 * ROWS, LANES)], axis=0
                )
                total = total + jnp.dot(
                    weights[16 + 4 * xx + pair_of], rows, preferred_element_type=F32
                )
            x_sum[xx] = total.astype(BF16)
        copies = [
            send(x_sum.at[wrap(x + k, NX)], x_in.at[k - 1], x_sum_sem, (k - 1,), (z, x_peers[k - 1]))
            for k in (2, 1, 3)
        ]
        sent.extend(copies)
        return copies

    def finish_last():
        for copy in x_sum_copies:
            copy.wait_recv()
        total = x_sum[x].astype(F32)
        for k in range(NX - 1):
            total = total + x_in[k].astype(F32)
        out_ref[last] = total.astype(BF16)

    def finish(q):
        for copy in to_y[q]:
            copy.wait_recv()
        total = summed[q, y].astype(F32)
        for k in range(NY - 1):
            total = total + y_in[q, k].astype(F32)
        out_ref[q] = total.astype(BF16)

    lane = lax.broadcasted_iota(jnp.int32, (8, LANES), 1)
    row = lax.broadcasted_iota(jnp.int32, (8, LANES), 0)

    def build(index, yy, column, first, second):
        chip = jnp.where(lane < LANES // 2, first, second)
        expert = (chip * 4 + lax.rem(lax.div(lane, ROWS), 4)).astype(F32)
        slot = lax.rem(lane, 2).astype(F32)
        tile = lax.rem(lax.div(lane, 2), 8)
        block = meta[yy, column]
        names = jnp.zeros((8, LANES), F32)
        gates = jnp.zeros((8, LANES), F32)
        for k in range(TOP):
            hit = block[:, k : k + 1] == expert
            names = names + jnp.where(hit, 1.0, 0.0)
            gates = gates + jnp.where(hit, block[:, TOP + k : TOP + k + 1], 0.0)
        earlier = shift_rows(names, 1, row)
        for by in (1, 2, 4):
            earlier = earlier + shift_rows(earlier, by, row)
        gates = jnp.where(earlier == slot, gates, 0.0)
        spread = jnp.concatenate([jnp.where(tile == j, gates, 0.0) for j in range(8)], axis=0)
        weights[index] = spread.astype(BF16)

    def square():
        def step(b, carry):
            yy, xx = lax.div(b, NX), lax.rem(b, NX)
            for e in range(4):
                total = jnp.zeros((8, LANES), F32)
                for q in range(chunks):
                    v = raw[q, e, yy, xx].astype(F32)
                    v = v * v
                    total = total + (v[:8] + v[8:])
                squares_of[yy, xx, e] = total
            return carry

        lax.fori_loop(0, NX * NY, step, 0)

    def count():
        expert = ((y * NX + x) * 4 + lane).astype(F32)
        odd = lax.rem(row, 2).astype(F32)

        def step(b, carry):
            yy, xx = lax.div(b, NX), lax.rem(b, NX)
            block = meta[yy, xx]
            names = jnp.zeros((8, LANES), F32)
            for k in range(TOP):
                names = names + jnp.where(block[:, k : k + 1] == expert, 1.0, 0.0)
            named = jnp.broadcast_to(jnp.sum(names, axis=0, keepdims=True), (8, LANES))
            squares, counts = list(carry[:4]), list(carry[4:])
            for e in range(4):
                much = jnp.broadcast_to(named[:, e : e + 1], (8, LANES))
                squares[e] = squares[e] + jnp.where(odd < much, squares_of[yy, xx, e], 0.0)
                counts[e] = counts[e] + much
            return (*squares, *counts)

        parts = lax.fori_loop(0, NX * NY, step, tuple(jnp.zeros((8, LANES), F32) for _ in range(8)))
        tile = jnp.zeros((8, LANES), F32)
        for e in range(4):
            total = jnp.sum(jnp.sum(parts[e], axis=0, keepdims=True), axis=1, keepdims=True)
            tile = jnp.where(row == e, jnp.broadcast_to(total, (8, LANES)), tile)
            tile = jnp.where(row == 4 + e, parts[4 + e], tile)
        stat[0] = tile

    me, chip_r, chip_l = y * NX + x, y * NX + xr, y * NX + xl
    send_far(0)
    y_raw_copies = send_y_raw()
    send_far(1)
    send_near(0)
    send_far(2)
    send_near(1)
    for q in range(3, last):
        own[q].wait()
        swap[q].wait_recv()
    square()
    for copy in meta_all:
        copy.wait_recv()
    for h in range(4):
        build(h, h, xr, me, chip_l)
        build(4 + h, 4 + h, xl, me, chip_r)
    send_comb(0)
    send_far(3)
    for h in range(4):
        build(8 + h, h, x, me, chip_r)
        build(12 + h, 4 + h, x, me, chip_l)
    send_comb(1)
    send_near(2)
    send_y(0)
    send_far(4)
    send_comb(2)
    send_near(3)
    count()
    pair = send(stat.at[0], stat_pair, pair_sem, (), (z, partner))
    sent.append(pair)
    send_y(1)
    send_far(5)
    send_comb(3)
    send_near(4)
    for xx in range(NX):
        for k in range(NY // 2):
            sources = [wrap(y + NY - j, NY) * NX + x for j in (2 * k, 2 * k + 1)]
            build(16 + 4 * xx + k, y, xx, *sources)
    send_y(2)
    send_comb(4)
    send_near(5)
    x_sum_copies = send_x_sum()
    send_comb(5)
    pair.wait_recv()
    stat[1] = stat[0] + stat_pair[...]
    to_z = [send(stat.at[1], stat_z.at[k], z_sem, (k,), (p, d)) for k, p in enumerate(z_peers)]
    sent += to_z
    finish(0)
    send_y(3)
    finish(1)
    send_y(4)
    finish(2)
    send_y(5)
    finish_last()
    finish(3)
    finish(4)
    for copy in to_z:
        copy.wait_recv()
    total = stat[1]
    for k in range(NZ - 1):
        total = total + stat_z[k]
    squares = jnp.where(c == 0, total[0:2], total[2:4])
    counts = jnp.where(c == 0, total[4:6], total[6:8])
    stat_ref[0:2] = jnp.sqrt(squares / (counts * float(chunks * 8 * LANES)) + EPS)
    stat_ref[2:4] = counts
    stat_ref[4:8] = jnp.zeros((4, LANES), F32)
    finish(5)
    for copy in sent:
        copy.wait_send()


def hand_over(in_ref, stat_ref, out_ref, counts_ref, rms_ref):
    out_ref[...] = in_ref[...]
    for e in range(2):
        rms_ref[e] = stat_ref[e, 0]
        counts_ref[e] = stat_ref[2 + e, 0].astype(jnp.int32)


def body(expert_out, expert_ids, gate_weight):
    width = expert_out.shape[4]
    tiles = width // LANES
    chunks = tiles // 8
    view = expert_out.reshape(2, NY, NX, 2, 2, tiles, LANES)
    view = view.transpose(0, 1, 2, 3, 5, 4, 6).reshape(2, NY, NX, 2, tiles * 2, LANES)
    def vmem(*shape):
        return pltpu.VMEM(shape, BF16)

    def dma(*shape):
        return pltpu.SemaphoreType.DMA(shape)

    half = (chunks, 4, 4, ROWS, LANES)
    done = (chunks, 4, TOK, LANES)
    out, stats = pl.pallas_call(
        lambda *refs: kernel(chunks, *refs),
        out_shape=(
            jax.ShapeDtypeStruct((chunks, TOK, LANES), BF16),
            jax.ShapeDtypeStruct((8, LANES), F32),
        ),
        in_specs=[
            pl.BlockSpec(memory_space=pltpu.HBM),
            pl.BlockSpec(memory_space=pltpu.VMEM),
            pl.BlockSpec(memory_space=pltpu.VMEM),
        ],
        out_specs=(pl.BlockSpec(memory_space=pltpu.VMEM), pl.BlockSpec(memory_space=pltpu.VMEM)),
        scratch_shapes=[
            vmem(chunks, 4, NY, NX, ROWS, LANES),
            vmem(*half), vmem(*half), vmem(*half), vmem(*half),
            vmem(*done), vmem(*done), vmem(*done), vmem(*done),
            vmem(chunks, NY, TOK, LANES), vmem(chunks, NY - 1, TOK, LANES),
            vmem(NY - 1, 4, NX, ROWS, LANES), vmem(NX, TOK, LANES), vmem(NX - 1, TOK, LANES),
            pltpu.VMEM((NY, NX, 8, LANES), F32), vmem(32, TOK, LANES),
            pltpu.VMEM((NY, NX, 4, 8, LANES), F32),
            pltpu.VMEM((2, 8, LANES), F32), pltpu.VMEM((8, LANES), F32),
            pltpu.VMEM((NZ - 1, 8, LANES), F32),
            dma(chunks), dma(2, chunks), dma(2, 2, chunks), dma(2, 2, chunks), dma(2, 2, chunks),
            dma(2, chunks, NY - 1), dma(2, NY - 1), dma(2, NX - 1), dma(2, NX * NY - 1), dma(2), dma(2, NZ - 1),
        ],
        compiler_params=pltpu.CompilerParams(
            collective_id=0, has_side_effects=True
        ),
    )(view, expert_ids, gate_weight)
    out, counts, rms = pl.pallas_call(
        hand_over,
        out_shape=(
            jax.ShapeDtypeStruct(out.shape, BF16),
            jax.ShapeDtypeStruct((2,), jnp.int32),
            jax.ShapeDtypeStruct((2,), F32),
        ),
        in_specs=[pl.BlockSpec(memory_space=pltpu.VMEM), pl.BlockSpec(memory_space=pltpu.VMEM)],
        out_specs=(
            pl.BlockSpec(memory_space=pltpu.VMEM),
            pl.BlockSpec(memory_space=pltpu.SMEM),
            pl.BlockSpec(memory_space=pltpu.SMEM),
        ),
    )(out, stats)
    combined = out.reshape(tiles, TOP, LANES).transpose(1, 0, 2).reshape(TOP, width)
    return combined, counts, rms


def solution(mesh):
    return jax.shard_map(
        body,
        mesh=mesh,
        in_specs=(
            P("dp", "expert", None, None, None),
            P(("dp", "expert"), None),
            P(("dp", "expert"), None),
        ),
        out_specs=(P(("dp", "expert"), None), P("expert"), P("expert")),
        check_vma=False,
    )
```

```python
import jax
import jax.numpy as jnp
from jax import lax
from jax.experimental import pallas as pl
from jax.experimental.pallas import tpu as pltpu
from jax.sharding import PartitionSpec as P

TOP = 8
NX, NY, NZ = 4, 8, 8
LANES = 128
ROWS = 16
TOK = 64
RING = 2
ORDER = (0, 5, 1, 6, 2, 3, 4)
EPS = 1e-06
MESH = pl.DeviceIdType.MESH
BF16, F32 = jnp.bfloat16, jnp.float32


def wrap(value, size):
    return lax.rem(value + size, size)


def shift_rows(v, by, row):
    return jnp.where(row >= by, pltpu.roll(v, by, 0), 0.0)


def kernel(
    chunks, x_ref, ids_ref, gates_ref, out_ref, stat_ref,
    raw, far_in, near_in, comb_out, comb_in, summed, y_in, ring_raw, ring_out, ring_in, x_sum, x_in,
    meta_rows, meta, weights, squares_of, stat, stat_pair, stat_z,
    loc_sem, swap_sem, far_sem, near_sem, comb_sem, y_sem, ring_raw_sem, ring_sem, x_sum_sem, small_sem, send_sem,
):
    z = lax.axis_index("dp")
    d = lax.axis_index("expert")
    c = lax.rem(d, 2)
    x = lax.rem(lax.div(d, 2), NX)
    y = lax.div(d, 2 * NX)
    xr, xl, xf = wrap(x + 1, NX), wrap(x + NX - 1, NX), wrap(x + 2, NX)

    def at(yy, xx, cc):
        return (yy * NX + xx) * 2 + cc

    count_x = chunks - RING
    partner, right, left = at(y, x, 1 - c), at(y, xr, c), at(y, xl, c)
    plane = [(i, j) for j in range(NX) for i in range(NY) if (i, j) != (0, 0)]
    peers = [at(wrap(y + i, NY), wrap(x + j, NX), c) for i, j in plane]
    x_peers = [at(y, wrap(x + k, NX), c) for k in range(1, NX)]
    y_peers = [at(wrap(y + k, NY), x, c) for k in range(1, NY)]
    z_peers = [wrap(z + k, NZ) for k in range(1, NZ)]
    sides, ahead = (right, left), (y_peers[0], y_peers[NY - 2])
    to_swap, to_far, to_near, to_comb, to_y, to_ring_raw, to_ring, to_x_sum, to_meta, to_pair, to_z = range(11)

    def send(src, dst, kind, arrival, device):
        pltpu.make_async_remote_copy(
            src_ref=src, dst_ref=dst, send_sem=send_sem.at[kind], recv_sem=arrival,
            device_id=device, device_id_type=MESH,
        ).start()

    def await_bytes(ref, sem):
        pltpu.make_async_copy(ref, ref, sem).wait()

    own = [
        pltpu.make_async_copy(
            x_ref.at[:, :, :, c, pl.ds(ROWS * q, ROWS), :], raw.at[q, pl.ds(2 * c, 2)], loc_sem.at[q]
        )
        for q in range(chunks)
    ]
    for copy in own:
        copy.start()

    lane = lax.broadcasted_iota(jnp.int32, (8, LANES), 1)
    row = lax.broadcasted_iota(jnp.int32, (8, LANES), 0)
    me_row = y * NX + x
    copies_of = jnp.where(lax.rem(lane, TOP) == row, 1.0, 0.0)
    named = jnp.dot(ids_ref[...].astype(F32), copies_of, preferred_element_type=F32)
    gated = jnp.dot(gates_ref[...], copies_of, preferred_element_type=F32)
    packed = jnp.where(lane < 8 * TOP, named, gated)
    packed = jnp.where(lax.rem(lax.div(lane, TOP), 8) == row, packed, 0.0)
    meta_rows[me_row] = jnp.sum(packed, axis=0, keepdims=True)

    barrier = pltpu.get_barrier_semaphore()
    greeted = [(z, partner)] + [(z, p) for p in peers] + [(p, d) for p in z_peers]
    for device in greeted:
        pl.semaphore_signal(barrier, inc=1, device_id=device, device_id_type=MESH)
    pl.semaphore_wait(barrier, len(greeted))

    for p in peers:
        send(meta_rows.at[me_row], meta_rows.at[me_row], to_meta, small_sem.at[0], (z, p))
    for q in ORDER:
        send(
            x_ref.at[:, :, :, 1 - c, pl.ds(ROWS * q, ROWS), :], raw.at[q, pl.ds(2 * c, 2)],
            to_swap, swap_sem.at[q], (z, partner),
        )

    def own_here(q):
        own[q].wait()

    def swap_here(q):
        await_bytes(raw.at[q, pl.ds(0, 2)], swap_sem.at[q])

    def send_far(q, first, amount):
        for side in range(2):
            send(
                raw.at[q, pl.ds(first, amount), pl.ds(4 * side, 4), xf],
                far_in.at[q, side, pl.ds(first, amount)],
                to_far, far_sem.at[q], (z, sides[side]),
            )

    def ring_row(step, way):
        return wrap(y + step if way == 0 else y + NY - step, NY)

    def ring_start(i, first, amount):
        for way in range(2):
            send(
                raw.at[count_x + i, pl.ds(first, amount), ring_row(4, way), pl.ds(2 * way, 2)],
                ring_raw.at[i, way, pl.ds(first, amount)],
                to_ring_raw, ring_raw_sem.at[i], (z, ahead[way]),
            )

    def send_near(q):
        for side in range(2):
            send(
                raw.at[q, :, pl.ds(4 - 4 * side, 4), (xr, xl)[side]], near_in.at[q, 1 - side],
                to_near, near_sem.at[q], (z, sides[side]),
            )

    def mixed(index, q, yy, column, other):
        rows = jnp.concatenate(
            [raw[q, :, yy, column].reshape(4 * ROWS, LANES), other.reshape(4 * ROWS, LANES)], axis=0
        )
        return jnp.dot(weights[index], rows, preferred_element_type=F32)

    def own_part(index, q, yy, xx):
        rows = raw[q, :, yy, xx].reshape(4 * ROWS, LANES)
        return jnp.dot(weights[index, :, 0:TOK], rows, preferred_element_type=F32)

    def send_comb(q):
        await_bytes(far_in.at[q], far_sem.at[q])
        for side in range(2):
            for h in range(4):
                total = mixed(4 * side + h, q, 4 * side + h, (xr, xl)[side], far_in[q, side, :, h])
                comb_out[q, side, h] = total.astype(BF16)
        for side in range(2):
            send(comb_out.at[q, side], comb_in.at[q, side], to_comb, comb_sem.at[q], (z, sides[side]))

    def send_y(q):
        await_bytes(near_in.at[q], near_sem.at[q])
        await_bytes(comb_in.at[q], comb_sem.at[q])
        for side in range(2):
            for h in range(4):
                total = mixed(8 + 4 * side + h, q, 4 * side + h, x, near_in[q, side, :, h])
                total = total + comb_in[q, side, h].astype(F32)
                summed[q, 4 * side + h] = total.astype(BF16)
        for k in (4, 3, 5, 2, 6, 1, 7):
            send(summed.at[q, wrap(y + k, NY)], y_in.at[q, k - 1], to_y, y_sem.at[q], (z, y_peers[k - 1]))

    def ring_step(i, step):
        q = count_x + i
        if step == 3:
            await_bytes(ring_raw.at[i], ring_raw_sem.at[i])
        else:
            await_bytes(ring_in.at[i, step], ring_sem.at[i, step])
        for way in range(2):
            yy = ring_row(step, way)
            for xx in range(NX):
                index = 16 + 8 * (step - 1) + 4 * way + xx
                if step < 3:
                    total = own_part(index, q, yy, xx) + ring_in[i, step, way, xx].astype(F32)
                elif xx // 2 == way:
                    total = mixed(index, q, yy, xx, ring_raw[i, way, :, xx % 2])
                else:
                    total = own_part(index, q, yy, xx)
                ring_out[i, step - 1, way, xx] = total.astype(BF16)
            send(
                ring_out.at[i, step - 1, way], ring_in.at[i, step - 1, way],
                to_ring, ring_sem.at[i, step - 1], (z, ahead[way]),
            )

    def send_x_sum(i):
        q = count_x + i
        await_bytes(ring_in.at[i, 0], ring_sem.at[i, 0])
        for xx in range(NX):
            total = own_part(40 + xx, q, y, xx)
            total = total + ring_in[i, 0, 0, xx].astype(F32) + ring_in[i, 0, 1, xx].astype(F32)
            x_sum[i, xx] = total.astype(BF16)
        for k in (2, 1, 3):
            send(
                x_sum.at[i, wrap(x + k, NX)], x_in.at[i, k - 1], to_x_sum, x_sum_sem.at[i],
                (z, x_peers[k - 1]),
            )

    def finish_ring(i):
        await_bytes(x_in.at[i], x_sum_sem.at[i])
        total = x_sum[i, x].astype(F32)
        for k in range(NX - 1):
            total = total + x_in[i, k].astype(F32)
        out_ref[count_x + i] = total.astype(BF16)

    def finish(q):
        await_bytes(y_in.at[q], y_sem.at[q])
        total = summed[q, y].astype(F32)
        for k in range(NY - 1):
            total = total + y_in[q, k].astype(F32)
        out_ref[q] = total.astype(BF16)

    def decode():
        rows = jnp.concatenate(
            [jnp.broadcast_to(meta_rows[b], (8, LANES)) for b in range(NX * NY)], axis=0
        )
        shape = (8 * NX * NY, LANES)
        token = lax.rem(lax.broadcasted_iota(jnp.int32, shape, 0), 8)
        place = lax.rem(lax.div(lax.broadcasted_iota(jnp.int32, shape, 1), TOP), 8)
        rows = jnp.where(token == place, rows, 0.0)
        source = lax.broadcasted_iota(jnp.int32, (LANES, LANES), 0)
        target = lax.broadcasted_iota(jnp.int32, (LANES, LANES), 1)
        kept = lax.rem(source, TOP) + TOP * lax.div(source, 8 * TOP) == target
        folded = jnp.dot(rows, jnp.where(kept, 1.0, 0.0), preferred_element_type=F32)
        meta[...] = folded.reshape(NY, NX, 8, LANES)

    def build(index, yy, column, first, second):
        chip = jnp.where(lane < LANES // 2, first, second)
        expert = (chip * 4 + lax.rem(lax.div(lane, ROWS), 4)).astype(F32)
        slot = lax.rem(lane, 2).astype(F32)
        tile = lax.rem(lax.div(lane, 2), 8)
        block = meta[yy, column]
        names = jnp.zeros((8, LANES), F32)
        gates = jnp.zeros((8, LANES), F32)
        for k in range(TOP):
            hit = block[:, k : k + 1] == expert
            names = names + jnp.where(hit, 1.0, 0.0)
            gates = gates + jnp.where(hit, block[:, TOP + k : TOP + k + 1], 0.0)
        earlier = shift_rows(names, 1, row)
        for by in (1, 2, 4):
            earlier = earlier + shift_rows(earlier, by, row)
        gates = jnp.where(earlier == slot, gates, 0.0)
        spread = jnp.concatenate([jnp.where(tile == j, gates, 0.0) for j in range(8)], axis=0)
        weights[index] = spread.astype(BF16)

    def square():
        def step(b, carry):
            yy, xx = lax.div(b, NX), lax.rem(b, NX)
            for e in range(4):
                total = jnp.zeros((8, LANES), F32)
                for q in range(chunks):
                    v = raw[q, e, yy, xx].astype(F32)
                    v = v * v
                    total = total + (v[:8] + v[8:])
                squares_of[e, b] = total
            return carry

        lax.fori_loop(0, NX * NY, step, 0)

    def count():
        total_rows = 8 * NX * NY
        blocks = meta[...].reshape(total_rows, LANES)
        column = lax.broadcasted_iota(jnp.int32, (total_rows, LANES), 1)
        odd = lax.rem(lax.broadcasted_iota(jnp.int32, (total_rows, LANES), 0), 2).astype(F32)
        group = lax.div(lax.broadcasted_iota(jnp.int32, (total_rows, total_rows), 0), 8)
        other = lax.div(lax.broadcasted_iota(jnp.int32, (total_rows, total_rows), 1), 8)
        same = jnp.where(group == other, 1.0, 0.0).astype(BF16)
        ones = jnp.ones((LANES, LANES), BF16)
        ids = jnp.where(column < TOP, blocks, -1.0)
        tile = jnp.zeros((8, LANES), F32)
        for e in range(4):
            expert = (me_row * 4 + e).astype(F32)
            hit = jnp.where(ids == expert, 1.0, 0.0).astype(BF16)
            by_token = jnp.dot(hit, ones, preferred_element_type=F32)
            named = jnp.dot(same, by_token.astype(BF16), preferred_element_type=F32)
            squares = squares_of[e].reshape(total_rows, LANES)
            squares = jnp.where(odd < named, squares, 0.0)
            total = jnp.sum(jnp.sum(squares, axis=0, keepdims=True), axis=1, keepdims=True)
            tile = jnp.where(row == e, jnp.broadcast_to(total, (8, LANES)), tile)
            seen = jnp.sum(by_token, axis=0, keepdims=True)
            tile = jnp.where(row == 4 + e, jnp.broadcast_to(seen, (8, LANES)), tile)
        stat[0] = tile
        send(stat.at[0], stat_pair, to_pair, small_sem.at[1], (z, partner))

    def share_stats():
        await_bytes(stat_pair, small_sem.at[1])
        stat[1] = stat[0] + stat_pair[...]
        for k, p in enumerate(z_peers):
            send(stat.at[1], stat_z.at[k], to_z, small_sem.at[2], (p, d))

    def finish_stats():
        await_bytes(stat_z, small_sem.at[2])
        total = stat[1]
        for k in range(NZ - 1):
            total = total + stat_z[k]
        squares = jnp.where(c == 0, total[0:2], total[2:4])
        counts = jnp.where(c == 0, total[4:6], total[6:8])
        stat_ref[0:2] = jnp.sqrt(squares / (counts * float(chunks * 8 * LANES)) + EPS)
        stat_ref[2:4] = counts
        stat_ref[4:8] = jnp.zeros((4, LANES), F32)

    def build_near():
        for h in range(4):
            build(h, h, xr, me_row, y * NX + xl)
            build(4 + h, 4 + h, xl, me_row, y * NX + xr)

    def build_sum():
        for h in range(4):
            build(8 + h, h, x, me_row, y * NX + xr)
            build(12 + h, 4 + h, x, me_row, y * NX + xl)

    def build_ring(step):
        for way in range(2):
            behind = wrap(y + NY - 1 if way == 0 else y + 1, NY) * NX + x
            for xx in range(NX):
                build(16 + 8 * (step - 1) + 4 * way + xx, ring_row(step, way), xx, me_row, behind)

    def build_x_sum():
        for xx in range(NX):
            build(40 + xx, y, xx, me_row, me_row)

    def await_meta():
        await_bytes(meta_rows.at[pl.ds(0, NX * NY - 1)], small_sem.at[0])

    def await_sent():
        await_bytes(x_ref.at[:, :, :, 0], send_sem.at[to_swap])
        for ref, kind in (
            (far_in, to_far), (near_in, to_near), (comb_in, to_comb), (y_in, to_y), (ring_raw, to_ring_raw),
            (ring_in, to_ring), (x_in, to_x_sum), (meta_rows.at[pl.ds(0, NX * NY - 1)], to_meta),
            (stat_pair, to_pair), (stat_z, to_z),
        ):
            await_bytes(ref, send_sem.at[kind])

    mine, others = 2 * c, 2 - 2 * c
    for q in range(3):
        own_here(q)
        send_far(q, mine, 2)
    for i in range(RING):
        own_here(count_x + i)
        ring_start(i, mine, 2)
    for q in ORDER:
        swap_here(q)
        if q < 3:
            send_far(q, others, 2)
        elif q < count_x:
            own_here(q)
            send_far(q, 0, 4)
        else:
            ring_start(q - count_x, others, 2)
    send_near(0)
    square()
    await_meta()
    decode()
    build_near()
    send_comb(0)
    build_ring(3)
    for i in range(RING):
        ring_step(i, 3)
    send_near(1)
    send_comb(1)
    send_near(2)
    send_comb(2)
    build_ring(2)
    build_sum()
    send_near(3)
    send_comb(3)
    send_near(4)
    send_comb(4)
    build_ring(1)
    build_x_sum()
    ring_step(0, 2)
    send_y(0)
    ring_step(1, 2)
    count()
    send_y(1)
    ring_step(0, 1)
    ring_step(1, 1)
    share_stats()
    send_y(2)
    send_y(3)
    send_x_sum(0)
    send_x_sum(1)
    finish(0)
    send_y(4)
    finish(1)
    finish_ring(0)
    finish_ring(1)
    finish(2)
    finish_stats()
    finish(3)
    finish(4)
    await_sent()


def hand_over(in_ref, stat_ref, out_ref, counts_ref, rms_ref):
    out_ref[...] = in_ref[...]
    for e in range(2):
        rms_ref[e] = stat_ref[e, 0]
        counts_ref[e] = stat_ref[2 + e, 0].astype(jnp.int32)


def body(expert_out, expert_ids, gate_weight):
    width = expert_out.shape[4]
    tiles = width // LANES
    chunks = tiles // 8
    view = expert_out.reshape(2, NY, NX, 2, 2, tiles, LANES)
    view = view.transpose(0, 1, 2, 3, 5, 4, 6).reshape(2, NY, NX, 2, tiles * 2, LANES)
    def vmem(*shape):
        return pltpu.VMEM(shape, BF16)

    def dma(*shape):
        return pltpu.SemaphoreType.DMA(shape)

    half = (chunks - RING, 2, 4, 4, ROWS, LANES)
    done = (chunks - RING, 2, 4, TOK, LANES)
    ring = (RING, 3, 2, NX, TOK, LANES)
    out, stats = pl.pallas_call(
        lambda *refs: kernel(chunks, *refs),
        out_shape=(
            jax.ShapeDtypeStruct((chunks, TOK, LANES), BF16),
            jax.ShapeDtypeStruct((8, LANES), F32),
        ),
        in_specs=[
            pl.BlockSpec(memory_space=pltpu.HBM),
            pl.BlockSpec(memory_space=pltpu.VMEM),
            pl.BlockSpec(memory_space=pltpu.VMEM),
        ],
        out_specs=(pl.BlockSpec(memory_space=pltpu.VMEM), pl.BlockSpec(memory_space=pltpu.VMEM)),
        scratch_shapes=[
            vmem(chunks, 4, NY, NX, ROWS, LANES),
            vmem(*half), vmem(*half), vmem(*done), vmem(*done),
            vmem(chunks - RING, NY, TOK, LANES), vmem(chunks - RING, NY - 1, TOK, LANES),
            vmem(RING, 2, 4, 2, ROWS, LANES), vmem(*ring), vmem(*ring),
            vmem(RING, NX, TOK, LANES), vmem(RING, NX - 1, TOK, LANES),
            pltpu.VMEM((NY * NX, 1, LANES), F32), pltpu.VMEM((NY, NX, 8, LANES), F32),
            vmem(44, TOK, LANES), pltpu.VMEM((4, NY * NX, 8, LANES), F32),
            pltpu.VMEM((2, 8, LANES), F32), pltpu.VMEM((8, LANES), F32),
            pltpu.VMEM((NZ - 1, 8, LANES), F32),
            dma(chunks), dma(chunks), dma(chunks - RING), dma(chunks - RING), dma(chunks - RING),
            dma(chunks - RING), dma(RING), dma(RING, 3), dma(RING), dma(3), dma(11),
        ],
        compiler_params=pltpu.CompilerParams(
            collective_id=0, has_side_effects=True
        ),
    )(view, expert_ids, gate_weight)
    out, counts, rms = pl.pallas_call(
        hand_over,
        out_shape=(
            jax.ShapeDtypeStruct(out.shape, BF16),
            jax.ShapeDtypeStruct((2,), jnp.int32),
            jax.ShapeDtypeStruct((2,), F32),
        ),
        in_specs=[pl.BlockSpec(memory_space=pltpu.VMEM), pl.BlockSpec(memory_space=pltpu.VMEM)],
        out_specs=(
            pl.BlockSpec(memory_space=pltpu.VMEM),
            pl.BlockSpec(memory_space=pltpu.SMEM),
            pl.BlockSpec(memory_space=pltpu.SMEM),
        ),
    )(out, stats)
    combined = out.reshape(tiles, TOP, LANES).transpose(1, 0, 2).reshape(TOP, width)
    return combined, counts, rms


def solution(mesh):
    return jax.shard_map(
        body,
        mesh=mesh,
        in_specs=(
            P("dp", "expert", None, None, None),
            P(("dp", "expert"), None),
            P(("dp", "expert"), None),
        ),
        out_specs=(P(("dp", "expert"), None), P("expert"), P("expert")),
        check_vma=False,
    )
```

```python
import jax
import jax.numpy as jnp
from jax import lax
from jax.experimental import pallas as pl
from jax.experimental.pallas import tpu as pltpu
from jax.sharding import PartitionSpec as P

TOP = 8
NX, NY, NZ = 4, 8, 8
LANES = 128
ROWS = 16
TOK = 64
RING = 3
ORDER = (0, 4, 1, 5, 2, 6, 3)
EPS = 1e-06
MESH = pl.DeviceIdType.MESH
BF16, F32 = jnp.bfloat16, jnp.float32


def wrap(value, size):
    return lax.rem(value + size, size)


def shift_rows(v, by, row):
    return jnp.where(row >= by, pltpu.roll(v, by, 0), 0.0)


def kernel(
    chunks, x_ref, ids_hbm, gates_hbm, out_ref, stat_ref,
    raw, far_in, near_in, comb_out, comb_in, summed, via_in, via_out, y_in, ring_raw, ring_next, ring_half, ring_out, ring_in, x_sum, x_in,
    ids_ref, gates_ref, meta_rows, meta, weights, squares_of, stat, stat_pair, stat_z,
    loc_sem, swap_sem, far_sem, near_sem, comb_sem, via_sem, y_sem, ring_raw_sem, ring_sem, x_sum_sem, small_sem, send_sem, arg_sem,
):
    z = lax.axis_index("dp")
    d = lax.axis_index("expert")
    c = lax.rem(d, 2)
    x = lax.rem(lax.div(d, 2), NX)
    y = lax.div(d, 2 * NX)
    xr, xl, xf = wrap(x + 1, NX), wrap(x + NX - 1, NX), wrap(x + 2, NX)

    def at(yy, xx, cc):
        return (yy * NX + xx) * 2 + cc

    count_x = chunks - RING
    partner, right, left = at(y, x, 1 - c), at(y, xr, c), at(y, xl, c)
    plane = [(i, j) for j in range(NX) for i in range(NY) if (i, j) != (0, 0)]
    peers = [at(wrap(y + i, NY), wrap(x + j, NX), c) for i, j in plane]
    x_peers = [at(y, wrap(x + k, NX), c) for k in range(1, NX)]
    y_peers = [at(wrap(y + k, NY), x, c) for k in range(1, NY)]
    z_peers = [wrap(z + k, NZ) for k in range(1, NZ)]
    sides, ahead = (right, left), (y_peers[0], y_peers[NY - 2])
    to_swap, to_far, to_near, to_comb, to_y, to_ring_raw, to_ring, to_x_sum, to_meta, to_pair, to_z = range(11)
    to_via, to_ring_next, to_ring_half = range(11, 14)

    def send(src, dst, kind, arrival, device):
        pltpu.make_async_remote_copy(
            src_ref=src, dst_ref=dst, send_sem=send_sem.at[kind], recv_sem=arrival,
            device_id=device, device_id_type=MESH,
        ).start()

    def await_bytes(ref, sem):
        pltpu.make_async_copy(ref, ref, sem).wait()

    own = [
        pltpu.make_async_copy(
            x_ref.at[:, :, :, c, pl.ds(ROWS * q, ROWS), :], raw.at[q, pl.ds(2 * c, 2)], loc_sem.at[q]
        )
        for q in range(chunks)
    ]
    given = [
        pltpu.make_async_copy(ids_hbm, ids_ref, arg_sem.at[0]),
        pltpu.make_async_copy(gates_hbm, gates_ref, arg_sem.at[1]),
    ]
    for copy in given:
        copy.start()
    barrier = pltpu.get_barrier_semaphore()
    greeted = [(z, partner)] + [(z, p) for p in peers] + [(p, d) for p in z_peers]
    for device in greeted:
        pl.semaphore_signal(barrier, inc=1, device_id=device, device_id_type=MESH)
    for copy in own:
        copy.start()
    for copy in given:
        copy.wait()

    lane = lax.broadcasted_iota(jnp.int32, (8, LANES), 1)
    row = lax.broadcasted_iota(jnp.int32, (8, LANES), 0)
    me_row = y * NX + x
    copies_of = jnp.where(lax.rem(lane, TOP) == row, 1.0, 0.0)
    named = jnp.dot(ids_ref[...].astype(F32), copies_of, preferred_element_type=F32)
    gated = jnp.dot(gates_ref[...], copies_of, preferred_element_type=F32)
    packed = jnp.where(lane < 8 * TOP, named, gated)
    packed = jnp.where(lax.rem(lax.div(lane, TOP), 8) == row, packed, 0.0)
    meta_rows[me_row] = jnp.sum(packed, axis=0, keepdims=True)
    pl.semaphore_wait(barrier, len(greeted))

    for p in peers:
        send(meta_rows.at[me_row], meta_rows.at[me_row], to_meta, small_sem.at[0], (z, p))
    for q in ORDER:
        send(
            x_ref.at[:, :, :, 1 - c, pl.ds(ROWS * q, ROWS), :], raw.at[q, pl.ds(2 * c, 2)],
            to_swap, swap_sem.at[q], (z, partner),
        )

    def own_here(q):
        own[q].wait()

    def swap_here(q):
        await_bytes(raw.at[q, pl.ds(0, 2)], swap_sem.at[q])

    def send_far(q, first, amount):
        for side in range(2):
            send(
                raw.at[q, pl.ds(first, amount), pl.ds(4 * side, 4), xf],
                far_in.at[q, side, pl.ds(first, amount)],
                to_far, far_sem.at[q], (z, sides[side]),
            )

    def ring_row(step, way):
        return wrap(y + step if way == 0 else y + NY - step, NY)

    def ring_start(i, first, amount):
        for way in range(2):
            send(
                raw.at[count_x + i, pl.ds(first, amount), ring_row(4, way), pl.ds(2 * way, 2)],
                ring_raw.at[i, way, pl.ds(first, amount)],
                to_ring_raw, ring_raw_sem.at[i, 0], (z, ahead[way]),
            )

    def ring_more(i):
        for way in range(2):
            send(
                raw.at[count_x + i, :, ring_row(3, way), pl.ds(2 - 2 * way, 2)], ring_next.at[i, way],
                to_ring_next, ring_raw_sem.at[i, 1], (z, ahead[way]),
            )

    def send_near(q):
        for side in range(2):
            send(
                raw.at[q, :, pl.ds(4 - 4 * side, 4), (xr, xl)[side]], near_in.at[q, 1 - side],
                to_near, near_sem.at[q], (z, sides[side]),
            )

    def mixed(index, q, yy, column, other):
        rows = jnp.concatenate(
            [raw[q, :, yy, column].reshape(4 * ROWS, LANES), other.reshape(4 * ROWS, LANES)], axis=0
        )
        return jnp.dot(weights[index], rows, preferred_element_type=F32)

    def own_part(index, q, yy, xx):
        rows = raw[q, :, yy, xx].reshape(4 * ROWS, LANES)
        return jnp.dot(weights[index, :, 0:TOK], rows, preferred_element_type=F32)

    def send_comb(q):
        await_bytes(far_in.at[q], far_sem.at[q])
        for side in range(2):
            for h in range(4):
                total = mixed(4 * side + h, q, 4 * side + h, (xr, xl)[side], far_in[q, side, :, h])
                comb_out[q, side, h] = total.astype(BF16)
        for side in range(2):
            send(comb_out.at[q, side], comb_in.at[q, side], to_comb, comb_sem.at[q], (z, sides[side]))

    def send_y(q):
        await_bytes(near_in.at[q], near_sem.at[q])
        await_bytes(comb_in.at[q], comb_sem.at[q])
        for side in range(2):
            for h in range(4):
                total = mixed(8 + 4 * side + h, q, 4 * side + h, x, near_in[q, side, :, h])
                total = total + comb_in[q, side, h].astype(F32)
                summed[q, 4 * side + h] = total.astype(BF16)
        for way in range(2):
            next_to, beyond = (z, ahead[way]), (z, y_peers[1 if way == 0 else NY - 3])
            send(
                summed.at[q, ring_row(4, way), pl.ds(TOK // 2 * way, TOK // 2)],
                via_in.at[q, way, pl.ds(TOK, TOK // 2)], to_via, via_sem.at[q], beyond,
            )
            send(
                summed.at[q, ring_row(3, way)], via_in.at[q, way, pl.ds(0, TOK)],
                to_via, via_sem.at[q], next_to,
            )
        for way in range(2):
            send(
                summed.at[q, ring_row(1, way)], y_in.at[q, way, 0],
                to_y, y_sem.at[q], (z, ahead[way]),
            )

    def pass_on(q):
        await_bytes(via_in.at[q], via_sem.at[q])
        edge = TOK // 2
        for way in range(2):
            total = summed[q, ring_row(2, way)].astype(F32) + via_in[q, way, 0:TOK].astype(F32)
            more = via_in[q, way, TOK : TOK + edge].astype(F32)
            low, high = total[0:edge], total[edge:TOK]
            low, high = (low + more, high) if way == 0 else (low, high + more)
            via_out[q, way, 0:edge] = low.astype(BF16)
            via_out[q, way, edge:TOK] = high.astype(BF16)
            send(
                via_out.at[q, way], y_in.at[q, way, 1],
                to_y, y_sem.at[q], (z, y_peers[1 if way == 0 else NY - 3]),
            )

    def ring_step(i, step):
        q = count_x + i
        if step == 3:
            await_bytes(ring_raw.at[i], ring_raw_sem.at[i, 0])
        elif step == 2:
            await_bytes(ring_half.at[i], ring_sem.at[i, 2])
            await_bytes(ring_next.at[i], ring_raw_sem.at[i, 1])
        else:
            await_bytes(ring_in.at[i, 1], ring_sem.at[i, 1])
        for way in range(2):
            yy = ring_row(step, way)
            for xx in range(NX):
                index = 16 + 8 * (step - 1) + 4 * way + xx
                paired = xx // 2 == way
                if step == 3 and not paired:
                    continue
                if step == 3:
                    total = mixed(index, q, yy, xx, ring_raw[i, way, :, xx % 2])
                elif step == 2 and not paired:
                    total = mixed(index, q, yy, xx, ring_next[i, way, :, xx % 2])
                elif step == 2:
                    total = own_part(index, q, yy, xx) + ring_half[i, way, xx % 2].astype(F32)
                else:
                    total = own_part(index, q, yy, xx) + ring_in[i, 1, way, xx].astype(F32)
                ring_out[i, step - 1, way, xx] = total.astype(BF16)
            if step == 3:
                send(
                    ring_out.at[i, 2, way, pl.ds(2 * way, 2)], ring_half.at[i, way],
                    to_ring_half, ring_sem.at[i, 2], (z, ahead[way]),
                )
            else:
                send(
                    ring_out.at[i, step - 1, way], ring_in.at[i, step - 1, way],
                    to_ring, ring_sem.at[i, step - 1], (z, ahead[way]),
                )

    def send_x_sum(i):
        q = count_x + i
        await_bytes(ring_in.at[i, 0], ring_sem.at[i, 0])
        for xx in range(NX):
            total = own_part(40 + xx, q, y, xx)
            total = total + ring_in[i, 0, 0, xx].astype(F32) + ring_in[i, 0, 1, xx].astype(F32)
            x_sum[i, xx] = total.astype(BF16)
        for k in (2, 1, 3):
            send(
                x_sum.at[i, wrap(x + k, NX)], x_in.at[i, k - 1], to_x_sum, x_sum_sem.at[i],
                (z, x_peers[k - 1]),
            )

    def finish_ring(i):
        await_bytes(x_in.at[i], x_sum_sem.at[i])
        total = x_sum[i, x].astype(F32)
        for k in range(NX - 1):
            total = total + x_in[i, k].astype(F32)
        out_ref[count_x + i] = total.astype(BF16)

    def finish(q):
        await_bytes(y_in.at[q], y_sem.at[q])
        total = summed[q, y].astype(F32)
        for way in range(2):
            total = total + y_in[q, way, 0].astype(F32) + y_in[q, way, 1].astype(F32)
        out_ref[q] = total.astype(BF16)

    def decode():
        rows = jnp.concatenate(
            [jnp.broadcast_to(meta_rows[b], (8, LANES)) for b in range(NX * NY)], axis=0
        )
        shape = (8 * NX * NY, LANES)
        token = lax.rem(lax.broadcasted_iota(jnp.int32, shape, 0), 8)
        place = lax.rem(lax.div(lax.broadcasted_iota(jnp.int32, shape, 1), TOP), 8)
        rows = jnp.where(token == place, rows, 0.0)
        source = lax.broadcasted_iota(jnp.int32, (LANES, LANES), 0)
        target = lax.broadcasted_iota(jnp.int32, (LANES, LANES), 1)
        kept = lax.rem(source, TOP) + TOP * lax.div(source, 8 * TOP) == target
        folded = jnp.dot(rows, jnp.where(kept, 1.0, 0.0), preferred_element_type=F32)
        meta[...] = folded.reshape(NY, NX, 8, LANES)

    def build(index, yy, column, first, second):
        chip = jnp.where(lane < LANES // 2, first, second)
        expert = (chip * 4 + lax.rem(lax.div(lane, ROWS), 4)).astype(F32)
        slot = lax.rem(lane, 2).astype(F32)
        tile = lax.rem(lax.div(lane, 2), 8)
        block = meta[yy, column]
        names = jnp.zeros((8, LANES), F32)
        gates = jnp.zeros((8, LANES), F32)
        for k in range(TOP):
            hit = block[:, k : k + 1] == expert
            names = names + jnp.where(hit, 1.0, 0.0)
            gates = gates + jnp.where(hit, block[:, TOP + k : TOP + k + 1], 0.0)
        earlier = shift_rows(names, 1, row)
        for by in (1, 2, 4):
            earlier = earlier + shift_rows(earlier, by, row)
        gates = jnp.where(earlier == slot, gates, 0.0)
        spread = jnp.concatenate([jnp.where(tile == j, gates, 0.0) for j in range(8)], axis=0)
        weights[index] = spread.astype(BF16)

    def square():
        def step(b, carry):
            yy, xx = lax.div(b, NX), lax.rem(b, NX)
            for e in range(4):
                total = jnp.zeros((8, LANES), F32)
                for q in range(chunks):
                    v = raw[q, e, yy, xx].astype(F32)
                    v = v * v
                    total = total + (v[:8] + v[8:])
                squares_of[e, b] = total
            return carry

        lax.fori_loop(0, NX * NY, step, 0)

    def count():
        total_rows = 8 * NX * NY
        blocks = meta[...].reshape(total_rows, LANES)
        column = lax.broadcasted_iota(jnp.int32, (total_rows, LANES), 1)
        odd = lax.rem(lax.broadcasted_iota(jnp.int32, (total_rows, LANES), 0), 2).astype(F32)
        group = lax.div(lax.broadcasted_iota(jnp.int32, (total_rows, total_rows), 0), 8)
        other = lax.div(lax.broadcasted_iota(jnp.int32, (total_rows, total_rows), 1), 8)
        same = jnp.where(group == other, 1.0, 0.0).astype(BF16)
        ones = jnp.ones((LANES, LANES), BF16)
        ids = jnp.where(column < TOP, blocks, -1.0)
        tile = jnp.zeros((8, LANES), F32)
        for e in range(4):
            expert = (me_row * 4 + e).astype(F32)
            hit = jnp.where(ids == expert, 1.0, 0.0).astype(BF16)
            by_token = jnp.dot(hit, ones, preferred_element_type=F32)
            named = jnp.dot(same, by_token.astype(BF16), preferred_element_type=F32)
            squares = squares_of[e].reshape(total_rows, LANES)
            squares = jnp.where(odd < named, squares, 0.0)
            total = jnp.sum(jnp.sum(squares, axis=0, keepdims=True), axis=1, keepdims=True)
            tile = jnp.where(row == e, jnp.broadcast_to(total, (8, LANES)), tile)
            seen = jnp.sum(by_token, axis=0, keepdims=True)
            tile = jnp.where(row == 4 + e, jnp.broadcast_to(seen, (8, LANES)), tile)
        stat[0] = tile
        send(stat.at[0], stat_pair, to_pair, small_sem.at[1], (z, partner))

    def share_stats():
        await_bytes(stat_pair, small_sem.at[1])
        stat[1] = stat[0] + stat_pair[...]
        for k, p in enumerate(z_peers):
            send(stat.at[1], stat_z.at[k], to_z, small_sem.at[2], (p, d))

    def finish_stats():
        await_bytes(stat_z, small_sem.at[2])
        total = stat[1]
        for k in range(NZ - 1):
            total = total + stat_z[k]
        squares = jnp.where(c == 0, total[0:2], total[2:4])
        counts = jnp.where(c == 0, total[4:6], total[6:8])
        stat_ref[0:2] = jnp.sqrt(squares / (counts * float(chunks * 8 * LANES)) + EPS)
        stat_ref[2:4] = counts
        stat_ref[4:8] = jnp.zeros((4, LANES), F32)

    def build_near():
        for h in range(4):
            build(h, h, xr, me_row, y * NX + xl)
            build(4 + h, 4 + h, xl, me_row, y * NX + xr)

    def build_sum():
        for h in range(4):
            build(8 + h, h, x, me_row, y * NX + xr)
            build(12 + h, 4 + h, x, me_row, y * NX + xl)

    def build_ring(step):
        for way in range(2):
            behind = wrap(y + NY - 1 if way == 0 else y + 1, NY) * NX + x
            for xx in range(NX):
                build(16 + 8 * (step - 1) + 4 * way + xx, ring_row(step, way), xx, me_row, behind)

    def build_x_sum():
        for xx in range(NX):
            build(40 + xx, y, xx, me_row, me_row)

    def await_meta():
        await_bytes(meta_rows.at[pl.ds(0, NX * NY - 1)], small_sem.at[0])

    def await_sent():
        await_bytes(x_ref.at[:, :, :, 0], send_sem.at[to_swap])
        for ref, kind in (
            (far_in, to_far), (near_in, to_near), (comb_in, to_comb), (y_in, to_y), (ring_raw, to_ring_raw),
            (ring_in, to_ring), (ring_next, to_ring_next), (ring_half, to_ring_half),
            (via_in, to_via), (x_in, to_x_sum), (meta_rows.at[pl.ds(0, NX * NY - 1)], to_meta),
            (stat_pair, to_pair), (stat_z, to_z),
        ):
            await_bytes(ref, send_sem.at[kind])

    mine, others = 2 * c, 2 - 2 * c
    for q in range(3):
        own_here(q)
        send_far(q, mine, 2)
    for i in range(RING):
        own_here(count_x + i)
        ring_start(i, mine, 2)
    for q in ORDER:
        swap_here(q)
        if q < 3:
            send_far(q, others, 2)
        elif q < count_x:
            own_here(q)
            send_far(q, 0, 4)
        else:
            ring_start(q - count_x, others, 2)
    for i in range(RING):
        ring_more(i)
    send_near(0)
    square()
    await_meta()
    decode()
    build_near()
    send_comb(0)
    build_ring(3)
    for i in range(RING):
        ring_step(i, 3)
    for q in range(1, count_x):
        send_near(q)
        send_comb(q)
    build_ring(2)
    build_sum()
    send_y(0)
    ring_step(0, 2)
    ring_step(1, 2)
    count()
    send_y(1)
    ring_step(2, 2)
    pass_on(0)
    build_ring(1)
    build_x_sum()
    ring_step(0, 1)
    share_stats()
    send_y(2)
    ring_step(1, 1)
    pass_on(1)
    send_y(3)
    ring_step(2, 1)
    pass_on(2)
    send_x_sum(0)
    send_x_sum(1)
    pass_on(3)
    finish_stats()
    finish(0)
    send_x_sum(2)
    finish(1)
    finish_ring(0)
    finish_ring(1)
    finish(2)
    finish_ring(2)
    finish(3)
    await_sent()


def hand_over(in_ref, stat_ref, out_ref, counts_ref, rms_ref):
    out_ref[...] = in_ref[...]
    for e in range(2):
        rms_ref[e] = stat_ref[e, 0]
        counts_ref[e] = stat_ref[2 + e, 0].astype(jnp.int32)


def body(expert_out, expert_ids, gate_weight):
    width = expert_out.shape[4]
    tiles = width // LANES
    chunks = tiles // 8
    view = expert_out.reshape(2, NY, NX, 2, 2, tiles, LANES)
    view = view.transpose(0, 1, 2, 3, 5, 4, 6).reshape(2, NY, NX, 2, tiles * 2, LANES)
    def vmem(*shape):
        return pltpu.VMEM(shape, BF16)

    def dma(*shape):
        return pltpu.SemaphoreType.DMA(shape)

    half = (chunks - RING, 2, 4, 4, ROWS, LANES)
    done = (chunks - RING, 2, 4, TOK, LANES)
    out, stats = pl.pallas_call(
        lambda *refs: kernel(chunks, *refs),
        out_shape=(
            jax.ShapeDtypeStruct((chunks, TOK, LANES), BF16),
            jax.ShapeDtypeStruct((8, LANES), F32),
        ),
        in_specs=[
            pl.BlockSpec(memory_space=pltpu.HBM),
            pl.BlockSpec(memory_space=pltpu.HBM),
            pl.BlockSpec(memory_space=pltpu.HBM),
        ],
        out_specs=(pl.BlockSpec(memory_space=pltpu.VMEM), pl.BlockSpec(memory_space=pltpu.VMEM)),
        scratch_shapes=[
            vmem(chunks, 4, NY, NX, ROWS, LANES),
            vmem(*half), vmem(*half), vmem(*done), vmem(*done),
            vmem(chunks - RING, NY, TOK, LANES), vmem(chunks - RING, 2, TOK + TOK // 2, LANES),
            vmem(chunks - RING, 2, TOK, LANES), vmem(chunks - RING, 2, 2, TOK, LANES),
            vmem(RING, 2, 4, 2, ROWS, LANES), vmem(RING, 2, 4, 2, ROWS, LANES), vmem(RING, 2, 2, TOK, LANES),
            vmem(RING, 3, 2, NX, TOK, LANES), vmem(RING, 2, 2, NX, TOK, LANES),
            vmem(RING, NX, TOK, LANES), vmem(RING, NX - 1, TOK, LANES),
            pltpu.VMEM((TOP, TOP), jnp.int32), pltpu.VMEM((TOP, TOP), F32),
            pltpu.VMEM((NY * NX, 1, LANES), F32), pltpu.VMEM((NY, NX, 8, LANES), F32),
            vmem(44, TOK, LANES), pltpu.VMEM((4, NY * NX, 8, LANES), F32),
            pltpu.VMEM((2, 8, LANES), F32), pltpu.VMEM((8, LANES), F32),
            pltpu.VMEM((NZ - 1, 8, LANES), F32),
            dma(chunks), dma(chunks), dma(chunks - RING), dma(chunks - RING), dma(chunks - RING),
            dma(chunks - RING), dma(chunks - RING), dma(RING, 2), dma(RING, 3), dma(RING), dma(3), dma(14), dma(2),
        ],
        compiler_params=pltpu.CompilerParams(
            collective_id=0, has_side_effects=True
        ),
    )(view, expert_ids, gate_weight)
    out, counts, rms = pl.pallas_call(
        hand_over,
        out_shape=(
            jax.ShapeDtypeStruct(out.shape, BF16),
            jax.ShapeDtypeStruct((2,), jnp.int32),
            jax.ShapeDtypeStruct((2,), F32),
        ),
        in_specs=[pl.BlockSpec(memory_space=pltpu.VMEM), pl.BlockSpec(memory_space=pltpu.VMEM)],
        out_specs=(
            pl.BlockSpec(memory_space=pltpu.VMEM),
            pl.BlockSpec(memory_space=pltpu.SMEM),
            pl.BlockSpec(memory_space=pltpu.SMEM),
        ),
    )(out, stats)
    combined = out.reshape(tiles, TOP, LANES).transpose(1, 0, 2).reshape(TOP, width)
    return combined, counts, rms


def solution(mesh):
    return jax.shard_map(
        body,
        mesh=mesh,
        in_specs=(
            P("dp", "expert", None, None, None),
            P(("dp", "expert"), None),
            P(("dp", "expert"), None),
        ),
        out_specs=(P(("dp", "expert"), None), P("expert"), P("expert")),
        check_vma=False,
    )
```

```python
import jax
import jax.numpy as jnp
from jax import lax
from jax.experimental import pallas as pl
from jax.experimental.pallas import tpu as pltpu
from jax.sharding import PartitionSpec as P

TOP = 8
NX, NY, NZ = 4, 8, 8
LANES = 128
ROWS = 16
TOK = 64
RING = 3
ORDER = (0, 4, 1, 5, 2, 6, 3)
EPS = 1e-06
MESH = pl.DeviceIdType.MESH
BF16, F32 = jnp.bfloat16, jnp.float32


def wrap(value, size):
    return lax.rem(value + size, size)


def shift_rows(v, by, row):
    return jnp.where(row >= by, pltpu.roll(v, by, 0), 0.0)


def kernel(
    chunks, x_ref, ids_hbm, gates_hbm, out_ref, stat_ref,
    raw, far_in, near_in, comb_out, comb_in, summed, via_in, via_out, y_in, ring_raw, ring_next, ring_half, ring_out, ring_in, x_sum, x_in,
    ids_ref, gates_ref, meta_rows, meta, weights, squares_of, stat, stat_pair, stat_z,
    loc_sem, swap_sem, far_sem, near_sem, comb_sem, via_sem, y_sem, ring_raw_sem, ring_sem, x_sum_sem, small_sem, send_sem, arg_sem,
):
    z = lax.axis_index("dp")
    d = lax.axis_index("expert")
    c = lax.rem(d, 2)
    x = lax.rem(lax.div(d, 2), NX)
    y = lax.div(d, 2 * NX)
    xr, xl, xf = wrap(x + 1, NX), wrap(x + NX - 1, NX), wrap(x + 2, NX)

    def at(yy, xx, cc):
        return (yy * NX + xx) * 2 + cc

    count_x = chunks - RING
    partner, right, left = at(y, x, 1 - c), at(y, xr, c), at(y, xl, c)
    plane = [(i, j) for j in range(NX) for i in range(NY) if (i, j) != (0, 0)]
    plane.sort(key=lambda p: -(min(p[0], NY - p[0]) + min(p[1], NX - p[1])))
    peers = [at(wrap(y + i, NY), wrap(x + j, NX), c) for i, j in plane]
    x_peers = [at(y, wrap(x + k, NX), c) for k in range(1, NX)]
    y_peers = [at(wrap(y + k, NY), x, c) for k in range(1, NY)]
    z_peers = [wrap(z + k, NZ) for k in range(1, NZ)]
    sides, ahead = (right, left), (y_peers[0], y_peers[NY - 2])
    to_swap, to_far, to_near, to_comb, to_y, to_ring_raw, to_ring, to_x_sum, to_meta, to_pair, to_z = range(11)
    to_via, to_ring_next, to_ring_half = range(11, 14)

    def send(src, dst, kind, arrival, device):
        pltpu.make_async_remote_copy(
            src_ref=src, dst_ref=dst, send_sem=send_sem.at[kind], recv_sem=arrival,
            device_id=device, device_id_type=MESH,
        ).start()

    def await_bytes(ref, sem):
        pltpu.make_async_copy(ref, ref, sem).wait()

    own = [
        pltpu.make_async_copy(
            x_ref.at[:, :, :, c, pl.ds(ROWS * q, ROWS), :], raw.at[q, pl.ds(2 * c, 2)], loc_sem.at[q]
        )
        for q in range(chunks)
    ]
    given = [
        pltpu.make_async_copy(ids_hbm, ids_ref, arg_sem.at[0]),
        pltpu.make_async_copy(gates_hbm, gates_ref, arg_sem.at[1]),
    ]
    for copy in given:
        copy.start()
    barrier = pltpu.get_barrier_semaphore()
    greeted = [(z, partner)] + [(z, p) for p in peers] + [(p, d) for p in z_peers]
    for device in greeted:
        pl.semaphore_signal(barrier, inc=1, device_id=device, device_id_type=MESH)
    for copy in own:
        copy.start()
    for copy in given:
        copy.wait()

    lane = lax.broadcasted_iota(jnp.int32, (8, LANES), 1)
    row = lax.broadcasted_iota(jnp.int32, (8, LANES), 0)
    me_row = y * NX + x
    copies_of = jnp.where(lax.rem(lane, TOP) == row, 1.0, 0.0)
    named = jnp.dot(ids_ref[...].astype(F32), copies_of, preferred_element_type=F32)
    gated = jnp.dot(gates_ref[...], copies_of, preferred_element_type=F32)
    packed = jnp.where(lane < 8 * TOP, named, gated)
    packed = jnp.where(lax.rem(lax.div(lane, TOP), 8) == row, packed, 0.0)
    meta_rows[me_row] = jnp.sum(packed, axis=0, keepdims=True)
    pl.semaphore_wait(barrier, len(greeted))

    for p in peers:
        send(meta_rows.at[me_row], meta_rows.at[me_row], to_meta, small_sem.at[0], (z, p))
    for q in ORDER:
        send(
            x_ref.at[:, :, :, 1 - c, pl.ds(ROWS * q, ROWS), :], raw.at[q, pl.ds(2 * c, 2)],
            to_swap, swap_sem.at[q], (z, partner),
        )

    def own_here(q):
        own[q].wait()

    def swap_here(q):
        await_bytes(raw.at[q, pl.ds(0, 2)], swap_sem.at[q])

    def send_far(q, first, amount):
        for side in range(2):
            send(
                raw.at[q, pl.ds(first, amount), pl.ds(4 * side, 4), xf],
                far_in.at[q, side, pl.ds(first, amount)],
                to_far, far_sem.at[q], (z, sides[side]),
            )

    def ring_row(step, way):
        return wrap(y + step if way == 0 else y + NY - step, NY)

    def ring_start(i, first, amount):
        for way in range(2):
            send(
                raw.at[count_x + i, pl.ds(first, amount), ring_row(4, way), pl.ds(2 * way, 2)],
                ring_raw.at[i, way, pl.ds(first, amount)],
                to_ring_raw, ring_raw_sem.at[i, 0], (z, ahead[way]),
            )

    def ring_more(i):
        for way in range(2):
            send(
                raw.at[count_x + i, :, ring_row(3, way), pl.ds(2 - 2 * way, 2)], ring_next.at[i, way],
                to_ring_next, ring_raw_sem.at[i, 1], (z, ahead[way]),
            )

    def send_near(q):
        for side in range(2):
            send(
                raw.at[q, :, pl.ds(4 - 4 * side, 4), (xr, xl)[side]], near_in.at[q, 1 - side],
                to_near, near_sem.at[q], (z, sides[side]),
            )

    def mixed(index, q, yy, column, other):
        rows = jnp.concatenate(
            [raw[q, :, yy, column].reshape(4 * ROWS, LANES), other.reshape(4 * ROWS, LANES)], axis=0
        )
        return jnp.dot(weights[index], rows, preferred_element_type=F32)

    def own_part(index, q, yy, xx):
        rows = raw[q, :, yy, xx].reshape(4 * ROWS, LANES)
        return jnp.dot(weights[index, :, 0:TOK], rows, preferred_element_type=F32)

    def send_comb(q):
        await_bytes(far_in.at[q], far_sem.at[q])
        for side in range(2):
            for h in range(4):
                total = mixed(4 * side + h, q, 4 * side + h, (xr, xl)[side], far_in[q, side, :, h])
                comb_out[q, side, h] = total.astype(BF16)
        for side in range(2):
            send(comb_out.at[q, side], comb_in.at[q, side], to_comb, comb_sem.at[q], (z, sides[side]))

    def send_y(q):
        await_bytes(near_in.at[q], near_sem.at[q])
        await_bytes(comb_in.at[q], comb_sem.at[q])
        for side in range(2):
            for h in range(4):
                total = mixed(8 + 4 * side + h, q, 4 * side + h, x, near_in[q, side, :, h])
                total = total + comb_in[q, side, h].astype(F32)
                summed[q, 4 * side + h] = total.astype(BF16)
        for way in range(2):
            next_to, beyond = (z, ahead[way]), (z, y_peers[1 if way == 0 else NY - 3])
            send(
                summed.at[q, ring_row(4, way), pl.ds(TOK // 2 * way, TOK // 2)],
                via_in.at[q, way, pl.ds(TOK, TOK // 2)], to_via, via_sem.at[q], beyond,
            )
            send(
                summed.at[q, ring_row(3, way)], via_in.at[q, way, pl.ds(0, TOK)],
                to_via, via_sem.at[q], next_to,
            )
        if q == count_x - 1:
            send_beside(q)

    def send_beside(q):
        for way in range(2):
            send(
                summed.at[q, ring_row(1, way)], y_in.at[q, way, 0],
                to_y, y_sem.at[q], (z, ahead[way]),
            )

    def pass_on(q):
        await_bytes(via_in.at[q], via_sem.at[q])
        edge = TOK // 2
        for way in range(2):
            total = summed[q, ring_row(2, way)].astype(F32) + via_in[q, way, 0:TOK].astype(F32)
            more = via_in[q, way, TOK : TOK + edge].astype(F32)
            low, high = total[0:edge], total[edge:TOK]
            low, high = (low + more, high) if way == 0 else (low, high + more)
            via_out[q, way, 0:edge] = low.astype(BF16)
            via_out[q, way, edge:TOK] = high.astype(BF16)
            send(
                via_out.at[q, way], y_in.at[q, way, 1],
                to_y, y_sem.at[q], (z, y_peers[1 if way == 0 else NY - 3]),
            )
        if q < count_x - 1:
            send_beside(q)

    def ring_step(i, step):
        q = count_x + i
        if step == 3:
            await_bytes(ring_raw.at[i], ring_raw_sem.at[i, 0])
        elif step == 2:
            await_bytes(ring_half.at[i], ring_sem.at[i, 2])
            await_bytes(ring_next.at[i], ring_raw_sem.at[i, 1])
        else:
            await_bytes(ring_in.at[i, 1], ring_sem.at[i, 1])
        for way in range(2):
            yy = ring_row(step, way)
            for xx in range(NX):
                index = 16 + 8 * (step - 1) + 4 * way + xx
                paired = xx // 2 == way
                if step == 3 and not paired:
                    continue
                if step == 3:
                    total = mixed(index, q, yy, xx, ring_raw[i, way, :, xx % 2])
                elif step == 2 and not paired:
                    total = mixed(index, q, yy, xx, ring_next[i, way, :, xx % 2])
                elif step == 2:
                    total = own_part(index, q, yy, xx) + ring_half[i, way, xx % 2].astype(F32)
                else:
                    total = own_part(index, q, yy, xx) + ring_in[i, 1, way, xx].astype(F32)
                ring_out[i, step - 1, way, xx] = total.astype(BF16)
            if step == 3:
                send(
                    ring_out.at[i, 2, way, pl.ds(2 * way, 2)], ring_half.at[i, way],
                    to_ring_half, ring_sem.at[i, 2], (z, ahead[way]),
                )
            else:
                send(
                    ring_out.at[i, step - 1, way], ring_in.at[i, step - 1, way],
                    to_ring, ring_sem.at[i, step - 1], (z, ahead[way]),
                )

    def send_x_sum(i):
        q = count_x + i
        await_bytes(ring_in.at[i, 0], ring_sem.at[i, 0])
        for xx in range(NX):
            total = own_part(40 + xx, q, y, xx)
            total = total + ring_in[i, 0, 0, xx].astype(F32) + ring_in[i, 0, 1, xx].astype(F32)
            x_sum[i, xx] = total.astype(BF16)
        for k in (2, 1, 3):
            send(
                x_sum.at[i, wrap(x + k, NX)], x_in.at[i, k - 1], to_x_sum, x_sum_sem.at[i],
                (z, x_peers[k - 1]),
            )

    def finish_ring(i):
        await_bytes(x_in.at[i], x_sum_sem.at[i])
        total = x_sum[i, x].astype(F32)
        for k in range(NX - 1):
            total = total + x_in[i, k].astype(F32)
        out_ref[count_x + i] = total.astype(BF16)

    def finish(q):
        await_bytes(y_in.at[q], y_sem.at[q])
        total = summed[q, y].astype(F32)
        for way in range(2):
            total = total + y_in[q, way, 0].astype(F32) + y_in[q, way, 1].astype(F32)
        out_ref[q] = total.astype(BF16)

    def decode():
        rows = jnp.concatenate(
            [jnp.broadcast_to(meta_rows[b], (8, LANES)) for b in range(NX * NY)], axis=0
        )
        shape = (8 * NX * NY, LANES)
        token = lax.rem(lax.broadcasted_iota(jnp.int32, shape, 0), 8)
        place = lax.rem(lax.div(lax.broadcasted_iota(jnp.int32, shape, 1), TOP), 8)
        rows = jnp.where(token == place, rows, 0.0)
        source = lax.broadcasted_iota(jnp.int32, (LANES, LANES), 0)
        target = lax.broadcasted_iota(jnp.int32, (LANES, LANES), 1)
        kept = lax.rem(source, TOP) + TOP * lax.div(source, 8 * TOP) == target
        folded = jnp.dot(rows, jnp.where(kept, 1.0, 0.0), preferred_element_type=F32)
        meta[...] = folded.reshape(NY, NX, 8, LANES)

    def build(index, yy, column, first, second):
        chip = jnp.where(lane < LANES // 2, first, second)
        expert = (chip * 4 + lax.rem(lax.div(lane, ROWS), 4)).astype(F32)
        slot = lax.rem(lane, 2).astype(F32)
        tile = lax.rem(lax.div(lane, 2), 8)
        block = meta[yy, column]
        names = jnp.zeros((8, LANES), F32)
        gates = jnp.zeros((8, LANES), F32)
        for k in range(TOP):
            hit = block[:, k : k + 1] == expert
            names = names + jnp.where(hit, 1.0, 0.0)
            gates = gates + jnp.where(hit, block[:, TOP + k : TOP + k + 1], 0.0)
        earlier = shift_rows(names, 1, row)
        for by in (1, 2, 4):
            earlier = earlier + shift_rows(earlier, by, row)
        gates = jnp.where(earlier == slot, gates, 0.0)
        spread = jnp.concatenate([jnp.where(tile == j, gates, 0.0) for j in range(8)], axis=0)
        weights[index] = spread.astype(BF16)

    def square():
        def step(b, carry):
            yy, xx = lax.div(b, NX), lax.rem(b, NX)
            for e in range(4):
                total = jnp.zeros((8, LANES), F32)
                for q in range(chunks):
                    v = raw[q, e, yy, xx].astype(F32)
                    v = v * v
                    total = total + (v[:8] + v[8:])
                squares_of[e, b] = total
            return carry

        lax.fori_loop(0, NX * NY, step, 0)

    def count():
        total_rows = 8 * NX * NY
        blocks = meta[...].reshape(total_rows, LANES)
        column = lax.broadcasted_iota(jnp.int32, (total_rows, LANES), 1)
        odd = lax.rem(lax.broadcasted_iota(jnp.int32, (total_rows, LANES), 0), 2).astype(F32)
        group = lax.div(lax.broadcasted_iota(jnp.int32, (total_rows, total_rows), 0), 8)
        other = lax.div(lax.broadcasted_iota(jnp.int32, (total_rows, total_rows), 1), 8)
        same = jnp.where(group == other, 1.0, 0.0).astype(BF16)
        ones = jnp.ones((LANES, LANES), BF16)
        ids = jnp.where(column < TOP, blocks, -1.0)
        tile = jnp.zeros((8, LANES), F32)
        for e in range(4):
            expert = (me_row * 4 + e).astype(F32)
            hit = jnp.where(ids == expert, 1.0, 0.0).astype(BF16)
            by_token = jnp.dot(hit, ones, preferred_element_type=F32)
            named = jnp.dot(same, by_token.astype(BF16), preferred_element_type=F32)
            squares = squares_of[e].reshape(total_rows, LANES)
            squares = jnp.where(odd < named, squares, 0.0)
            total = jnp.sum(jnp.sum(squares, axis=0, keepdims=True), axis=1, keepdims=True)
            tile = jnp.where(row == e, jnp.broadcast_to(total, (8, LANES)), tile)
            seen = jnp.sum(by_token, axis=0, keepdims=True)
            tile = jnp.where(row == 4 + e, jnp.broadcast_to(seen, (8, LANES)), tile)
        stat[0] = tile
        send(stat.at[0], stat_pair, to_pair, small_sem.at[1], (z, partner))

    def share_stats():
        await_bytes(stat_pair, small_sem.at[1])
        stat[1] = stat[0] + stat_pair[...]
        for k, p in enumerate(z_peers):
            send(stat.at[1], stat_z.at[k], to_z, small_sem.at[2], (p, d))

    def finish_stats():
        await_bytes(stat_z, small_sem.at[2])
        total = stat[1]
        for k in range(NZ - 1):
            total = total + stat_z[k]
        squares = jnp.where(c == 0, total[0:2], total[2:4])
        counts = jnp.where(c == 0, total[4:6], total[6:8])
        stat_ref[0:2] = jnp.sqrt(squares / (counts * float(chunks * 8 * LANES)) + EPS)
        stat_ref[2:4] = counts
        stat_ref[4:8] = jnp.zeros((4, LANES), F32)

    def build_near():
        for h in range(4):
            build(h, h, xr, me_row, y * NX + xl)
            build(4 + h, 4 + h, xl, me_row, y * NX + xr)

    def build_sum():
        for h in range(4):
            build(8 + h, h, x, me_row, y * NX + xr)
            build(12 + h, 4 + h, x, me_row, y * NX + xl)

    def build_ring(step):
        for way in range(2):
            behind = wrap(y + NY - 1 if way == 0 else y + 1, NY) * NX + x
            for xx in range(NX):
                build(16 + 8 * (step - 1) + 4 * way + xx, ring_row(step, way), xx, me_row, behind)

    def build_x_sum():
        for xx in range(NX):
            build(40 + xx, y, xx, me_row, me_row)

    def await_meta():
        await_bytes(meta_rows.at[pl.ds(0, NX * NY - 1)], small_sem.at[0])

    def await_sent():
        await_bytes(x_ref.at[:, :, :, 0], send_sem.at[to_swap])
        for ref, kind in (
            (far_in, to_far), (near_in, to_near), (comb_in, to_comb), (y_in, to_y), (ring_raw, to_ring_raw),
            (ring_in, to_ring), (ring_next, to_ring_next), (ring_half, to_ring_half),
            (via_in, to_via), (x_in, to_x_sum), (meta_rows.at[pl.ds(0, NX * NY - 1)], to_meta),
            (stat_pair, to_pair), (stat_z, to_z),
        ):
            await_bytes(ref, send_sem.at[kind])

    mine, others = 2 * c, 2 - 2 * c
    for q in range(3):
        own_here(q)
        send_far(q, mine, 2)
    for i in range(RING):
        own_here(count_x + i)
        ring_start(i, mine, 2)
    for q in ORDER:
        swap_here(q)
        if q < 3:
            send_far(q, others, 2)
        elif q < count_x:
            own_here(q)
            send_far(q, 0, 4)
        else:
            ring_start(q - count_x, others, 2)
    for i in range(RING):
        ring_more(i)
    send_near(0)
    square()
    await_meta()
    decode()
    build_near()
    send_comb(0)
    build_ring(3)
    for i in range(RING):
        ring_step(i, 3)
    for q in range(1, count_x):
        send_near(q)
        send_comb(q)
    build_ring(2)
    build_sum()
    send_y(0)
    ring_step(0, 2)
    ring_step(1, 2)
    count()
    send_y(1)
    ring_step(2, 2)
    pass_on(0)
    build_ring(1)
    build_x_sum()
    ring_step(0, 1)
    share_stats()
    send_y(2)
    ring_step(1, 1)
    pass_on(1)
    send_y(3)
    ring_step(2, 1)
    pass_on(2)
    send_x_sum(0)
    send_x_sum(1)
    pass_on(3)
    finish_stats()
    finish(0)
    send_x_sum(2)
    finish(1)
    finish_ring(0)
    finish_ring(1)
    finish(2)
    finish_ring(2)
    finish(3)
    await_sent()


def hand_over(in_ref, stat_ref, out_ref, counts_ref, rms_ref):
    out_ref[...] = in_ref[...]
    for e in range(2):
        rms_ref[e] = stat_ref[e, 0]
        counts_ref[e] = stat_ref[2 + e, 0].astype(jnp.int32)


def body(expert_out, expert_ids, gate_weight):
    width = expert_out.shape[4]
    tiles = width // LANES
    chunks = tiles // 8
    view = expert_out.reshape(2, NY, NX, 2, 2, tiles, LANES)
    view = view.transpose(0, 1, 2, 3, 5, 4, 6).reshape(2, NY, NX, 2, tiles * 2, LANES)
    def vmem(*shape):
        return pltpu.VMEM(shape, BF16)

    def dma(*shape):
        return pltpu.SemaphoreType.DMA(shape)

    half = (chunks - RING, 2, 4, 4, ROWS, LANES)
    done = (chunks - RING, 2, 4, TOK, LANES)
    out, stats = pl.pallas_call(
        lambda *refs: kernel(chunks, *refs),
        out_shape=(
            jax.ShapeDtypeStruct((chunks, TOK, LANES), BF16),
            jax.ShapeDtypeStruct((8, LANES), F32),
        ),
        in_specs=[
            pl.BlockSpec(memory_space=pltpu.HBM),
            pl.BlockSpec(memory_space=pltpu.HBM),
            pl.BlockSpec(memory_space=pltpu.HBM),
        ],
        out_specs=(pl.BlockSpec(memory_space=pltpu.VMEM), pl.BlockSpec(memory_space=pltpu.VMEM)),
        scratch_shapes=[
            vmem(chunks, 4, NY, NX, ROWS, LANES),
            vmem(*half), vmem(*half), vmem(*done), vmem(*done),
            vmem(chunks - RING, NY, TOK, LANES), vmem(chunks - RING, 2, TOK + TOK // 2, LANES),
            vmem(chunks - RING, 2, TOK, LANES), vmem(chunks - RING, 2, 2, TOK, LANES),
            vmem(RING, 2, 4, 2, ROWS, LANES), vmem(RING, 2, 4, 2, ROWS, LANES), vmem(RING, 2, 2, TOK, LANES),
            vmem(RING, 3, 2, NX, TOK, LANES), vmem(RING, 2, 2, NX, TOK, LANES),
            vmem(RING, NX, TOK, LANES), vmem(RING, NX - 1, TOK, LANES),
            pltpu.VMEM((TOP, TOP), jnp.int32), pltpu.VMEM((TOP, TOP), F32),
            pltpu.VMEM((NY * NX, 1, LANES), F32), pltpu.VMEM((NY, NX, 8, LANES), F32),
            vmem(44, TOK, LANES), pltpu.VMEM((4, NY * NX, 8, LANES), F32),
            pltpu.VMEM((2, 8, LANES), F32), pltpu.VMEM((8, LANES), F32),
            pltpu.VMEM((NZ - 1, 8, LANES), F32),
            dma(chunks), dma(chunks), dma(chunks - RING), dma(chunks - RING), dma(chunks - RING),
            dma(chunks - RING), dma(chunks - RING), dma(RING, 2), dma(RING, 3), dma(RING), dma(3), dma(14), dma(2),
        ],
        compiler_params=pltpu.CompilerParams(
            collective_id=0, has_side_effects=True, vmem_limit_bytes=54000 * 1024
        ),
    )(view, expert_ids, gate_weight)
    out, counts, rms = pl.pallas_call(
        hand_over,
        out_shape=(
            jax.ShapeDtypeStruct(out.shape, BF16),
            jax.ShapeDtypeStruct((2,), jnp.int32),
            jax.ShapeDtypeStruct((2,), F32),
        ),
        in_specs=[pl.BlockSpec(memory_space=pltpu.VMEM), pl.BlockSpec(memory_space=pltpu.VMEM)],
        out_specs=(
            pl.BlockSpec(memory_space=pltpu.VMEM),
            pl.BlockSpec(memory_space=pltpu.SMEM),
            pl.BlockSpec(memory_space=pltpu.SMEM),
        ),
        compiler_params=pltpu.CompilerParams(vmem_limit_bytes=32 * 1024 * 1024),
    )(out, stats)
    combined = out.reshape(tiles, TOP, LANES).transpose(1, 0, 2).reshape(TOP, width)
    return combined, counts, rms


def solution(mesh):
    return jax.shard_map(
        body,
        mesh=mesh,
        in_specs=(
            P("dp", "expert", None, None, None),
            P(("dp", "expert"), None),
            P(("dp", "expert"), None),
        ),
        out_specs=(P(("dp", "expert"), None), P("expert"), P("expert")),
        check_vma=False,
    )
```

```python
import jax
import jax.numpy as jnp
from jax import lax
from jax.experimental import pallas as pl
from jax.experimental.pallas import tpu as pltpu
from jax.sharding import PartitionSpec as P

TOP = 8
NX, NY, NZ = 4, 8, 8
LANES = 128
ROWS = 16
TOK = 64
RING = 3
ORDER = (0, 4, 1, 5, 2, 6, 3)
EPS = 1e-06
MESH = pl.DeviceIdType.MESH
BF16, F32 = jnp.bfloat16, jnp.float32


def wrap(value, size):
    return lax.rem(value + size, size)


def shift_rows(v, by, row):
    return jnp.where(row >= by, pltpu.roll(v, by, 0), 0.0)


def kernel(
    chunks, x_ref, ids_hbm, gates_hbm, out_ref, stat_ref,
    raw, far_in, near_in, comb_out, comb_in, summed, via_in, via_out, y_in, ring_raw, ring_next, ring_half, ring_out, ring_in, x_sum, x_in,
    ids_ref, gates_ref, meta_rows, meta, weights, squares_of, stat, stat_pair, stat_z,
    loc_sem, swap_sem, far_sem, near_sem, comb_sem, via_sem, y_sem, ring_raw_sem, ring_sem, x_sum_sem, small_sem, send_sem, arg_sem,
):
    z = lax.axis_index("dp")
    d = lax.axis_index("expert")
    c = lax.rem(d, 2)
    x = lax.rem(lax.div(d, 2), NX)
    y = lax.div(d, 2 * NX)
    xr, xl, xf = wrap(x + 1, NX), wrap(x + NX - 1, NX), wrap(x + 2, NX)

    def at(yy, xx, cc):
        return (yy * NX + xx) * 2 + cc

    count_x = chunks - RING
    partner, right, left = at(y, x, 1 - c), at(y, xr, c), at(y, xl, c)
    plane = [(i, j) for j in range(NX) for i in range(NY) if (i, j) != (0, 0)]
    plane.sort(key=lambda p: -(min(p[0], NY - p[0]) + min(p[1], NX - p[1])))
    peers = [at(wrap(y + i, NY), wrap(x + j, NX), c) for i, j in plane]
    x_peers = [at(y, wrap(x + k, NX), c) for k in range(1, NX)]
    y_peers = [at(wrap(y + k, NY), x, c) for k in range(1, NY)]
    z_peers = [wrap(z + k, NZ) for k in range(1, NZ)]
    sides, ahead = (right, left), (y_peers[0], y_peers[NY - 2])
    to_swap, to_far, to_near, to_comb, to_y, to_ring_raw, to_ring, to_x_sum, to_meta, to_pair, to_z = range(11)
    to_via, to_ring_next, to_ring_half = range(11, 14)

    def send(src, dst, kind, arrival, device):
        pltpu.make_async_remote_copy(
            src_ref=src, dst_ref=dst, send_sem=send_sem.at[kind], recv_sem=arrival,
            device_id=device, device_id_type=MESH,
        ).start()

    def await_bytes(ref, sem):
        pltpu.make_async_copy(ref, ref, sem).wait()

    own = [
        pltpu.make_async_copy(
            x_ref.at[:, :, :, c, pl.ds(ROWS * q, ROWS), :], raw.at[q, pl.ds(2 * c, 2)], loc_sem.at[q]
        )
        for q in range(chunks)
    ]
    given = [
        pltpu.make_async_copy(ids_hbm, ids_ref, arg_sem.at[0]),
        pltpu.make_async_copy(gates_hbm, gates_ref, arg_sem.at[1]),
    ]
    for copy in given:
        copy.start()
    barrier = pltpu.get_barrier_semaphore()
    greeted = [(z, partner)] + [(z, p) for p in peers] + [(p, d) for p in z_peers]
    for device in greeted:
        pl.semaphore_signal(barrier, inc=1, device_id=device, device_id_type=MESH)
    for copy in own:
        copy.start()
    for copy in given:
        copy.wait()

    lane = lax.broadcasted_iota(jnp.int32, (8, LANES), 1)
    row = lax.broadcasted_iota(jnp.int32, (8, LANES), 0)
    me_row = y * NX + x
    copies_of = jnp.where(lax.rem(lane, TOP) == row, 1.0, 0.0)
    named = jnp.dot(ids_ref[...].astype(F32), copies_of, preferred_element_type=F32)
    gated = jnp.dot(gates_ref[...], copies_of, preferred_element_type=F32)
    packed = jnp.where(lane < 8 * TOP, named, gated)
    packed = jnp.where(lax.rem(lax.div(lane, TOP), 8) == row, packed, 0.0)
    meta_rows[me_row] = jnp.sum(packed, axis=0, keepdims=True)
    pl.semaphore_wait(barrier, len(greeted))

    for p in peers:
        send(meta_rows.at[me_row], meta_rows.at[me_row], to_meta, small_sem.at[0], (z, p))
    for q in ORDER:
        send(
            x_ref.at[:, :, :, 1 - c, pl.ds(ROWS * q, ROWS), :], raw.at[q, pl.ds(2 * c, 2)],
            to_swap, swap_sem.at[q], (z, partner),
        )

    def own_here(q):
        own[q].wait()

    def swap_here(q):
        await_bytes(raw.at[q, pl.ds(0, 2)], swap_sem.at[q])

    def send_far(q, first, amount):
        for side in range(2):
            send(
                raw.at[q, pl.ds(first, amount), pl.ds(4 * side, 4), xf],
                far_in.at[q, side, pl.ds(first, amount)],
                to_far, far_sem.at[q], (z, sides[side]),
            )

    def ring_row(step, way):
        return wrap(y + step if way == 0 else y + NY - step, NY)

    def ring_start(i, first, amount):
        for way in range(2):
            send(
                raw.at[count_x + i, pl.ds(first, amount), ring_row(4, way), pl.ds(2 * way, 2)],
                ring_raw.at[i, way, pl.ds(first, amount)],
                to_ring_raw, ring_raw_sem.at[i, 0], (z, ahead[way]),
            )

    def ring_more(i):
        for way in range(2):
            send(
                raw.at[count_x + i, :, ring_row(3, way), pl.ds(2 - 2 * way, 2)], ring_next.at[i, way],
                to_ring_next, ring_raw_sem.at[i, 1], (z, ahead[way]),
            )

    def send_near(q):
        for side in range(2):
            send(
                raw.at[q, :, pl.ds(4 - 4 * side, 4), (xr, xl)[side]], near_in.at[q, 1 - side],
                to_near, near_sem.at[q], (z, sides[side]),
            )

    def mixed(index, q, yy, column, other):
        rows = jnp.concatenate(
            [raw[q, :, yy, column].reshape(4 * ROWS, LANES), other.reshape(4 * ROWS, LANES)], axis=0
        )
        return jnp.dot(weights[index], rows, preferred_element_type=F32)

    def own_part(index, q, yy, xx):
        rows = raw[q, :, yy, xx].reshape(4 * ROWS, LANES)
        return jnp.dot(weights[index, :, 0:TOK], rows, preferred_element_type=F32)

    def send_comb(q):
        await_bytes(far_in.at[q], far_sem.at[q])
        for side in range(2):
            for h in range(4):
                total = mixed(4 * side + h, q, 4 * side + h, (xr, xl)[side], far_in[q, side, :, h])
                comb_out[q, side, h] = total.astype(BF16)
        for side in range(2):
            send(comb_out.at[q, side], comb_in.at[q, side], to_comb, comb_sem.at[q], (z, sides[side]))

    def send_y(q):
        await_bytes(near_in.at[q], near_sem.at[q])
        await_bytes(comb_in.at[q], comb_sem.at[q])
        for side in range(2):
            for h in range(4):
                total = mixed(8 + 4 * side + h, q, 4 * side + h, x, near_in[q, side, :, h])
                total = total + comb_in[q, side, h].astype(F32)
                summed[q, 4 * side + h] = total.astype(BF16)
        for way in range(2):
            next_to, beyond = (z, ahead[way]), (z, y_peers[1 if way == 0 else NY - 3])
            send(
                summed.at[q, ring_row(4, way), pl.ds(TOK // 2 * way, TOK // 2)],
                via_in.at[q, way, pl.ds(TOK, TOK // 2)], to_via, via_sem.at[q], beyond,
            )
            send(
                summed.at[q, ring_row(3, way)], via_in.at[q, way, pl.ds(0, TOK)],
                to_via, via_sem.at[q], next_to,
            )
        if q == count_x - 1:
            send_beside(q)

    def send_beside(q):
        for way in range(2):
            send(
                summed.at[q, ring_row(1, way)], y_in.at[q, way, 0],
                to_y, y_sem.at[q], (z, ahead[way]),
            )

    def pass_on(q):
        await_bytes(via_in.at[q], via_sem.at[q])
        edge = TOK // 2
        for way in range(2):
            total = summed[q, ring_row(2, way)].astype(F32) + via_in[q, way, 0:TOK].astype(F32)
            more = via_in[q, way, TOK : TOK + edge].astype(F32)
            low, high = total[0:edge], total[edge:TOK]
            low, high = (low + more, high) if way == 0 else (low, high + more)
            via_out[q, way, 0:edge] = low.astype(BF16)
            via_out[q, way, edge:TOK] = high.astype(BF16)
            send(
                via_out.at[q, way], y_in.at[q, way, 1],
                to_y, y_sem.at[q], (z, y_peers[1 if way == 0 else NY - 3]),
            )
        if q < count_x - 1:
            send_beside(q)

    def ring_step(i, step):
        q = count_x + i
        if step == 3:
            await_bytes(ring_raw.at[i], ring_raw_sem.at[i, 0])
        elif step == 2:
            await_bytes(ring_half.at[i], ring_sem.at[i, 2])
            await_bytes(ring_next.at[i], ring_raw_sem.at[i, 1])
        else:
            await_bytes(ring_in.at[i, 1], ring_sem.at[i, 1])
        for way in range(2):
            yy = ring_row(step, way)
            for xx in range(NX):
                index = 16 + 8 * (step - 1) + 4 * way + xx
                paired = xx // 2 == way
                if step == 3 and not paired:
                    continue
                if step == 3:
                    total = mixed(index, q, yy, xx, ring_raw[i, way, :, xx % 2])
                elif step == 2 and not paired:
                    total = mixed(index, q, yy, xx, ring_next[i, way, :, xx % 2])
                elif step == 2:
                    total = own_part(index, q, yy, xx) + ring_half[i, way, xx % 2].astype(F32)
                else:
                    total = own_part(index, q, yy, xx) + ring_in[i, 1, way, xx].astype(F32)
                ring_out[i, step - 1, way, xx] = total.astype(BF16)
            if step == 3:
                send(
                    ring_out.at[i, 2, way, pl.ds(2 * way, 2)], ring_half.at[i, way],
                    to_ring_half, ring_sem.at[i, 2], (z, ahead[way]),
                )
            else:
                send(
                    ring_out.at[i, step - 1, way], ring_in.at[i, step - 1, way],
                    to_ring, ring_sem.at[i, step - 1], (z, ahead[way]),
                )

    def send_x_sum(i):
        q = count_x + i
        await_bytes(ring_in.at[i, 0], ring_sem.at[i, 0])
        for xx in range(NX):
            total = own_part(40 + xx, q, y, xx)
            total = total + ring_in[i, 0, 0, xx].astype(F32) + ring_in[i, 0, 1, xx].astype(F32)
            x_sum[i, xx] = total.astype(BF16)
        for k in (2, 1, 3):
            send(
                x_sum.at[i, wrap(x + k, NX)], x_in.at[i, k - 1], to_x_sum, x_sum_sem.at[i],
                (z, x_peers[k - 1]),
            )

    def finish_ring(i):
        await_bytes(x_in.at[i], x_sum_sem.at[i])
        total = x_sum[i, x].astype(F32)
        for k in range(NX - 1):
            total = total + x_in[i, k].astype(F32)
        out_ref[count_x + i] = total.astype(BF16)

    def finish(q):
        await_bytes(y_in.at[q], y_sem.at[q])
        total = summed[q, y].astype(F32)
        for way in range(2):
            total = total + y_in[q, way, 0].astype(F32) + y_in[q, way, 1].astype(F32)
        out_ref[q] = total.astype(BF16)

    def decode():
        rows = jnp.concatenate(
            [jnp.broadcast_to(meta_rows[b], (8, LANES)) for b in range(NX * NY)], axis=0
        )
        shape = (8 * NX * NY, LANES)
        token = lax.rem(lax.broadcasted_iota(jnp.int32, shape, 0), 8)
        place = lax.rem(lax.div(lax.broadcasted_iota(jnp.int32, shape, 1), TOP), 8)
        rows = jnp.where(token == place, rows, 0.0)
        source = lax.broadcasted_iota(jnp.int32, (LANES, LANES), 0)
        target = lax.broadcasted_iota(jnp.int32, (LANES, LANES), 1)
        kept = lax.rem(source, TOP) + TOP * lax.div(source, 8 * TOP) == target
        folded = jnp.dot(rows, jnp.where(kept, 1.0, 0.0), preferred_element_type=F32)
        meta[...] = folded.reshape(NY, NX, 8, LANES)

    def build(index, yy, column, first, second):
        chip = jnp.where(lane < LANES // 2, first, second)
        expert = (chip * 4 + lax.rem(lax.div(lane, ROWS), 4)).astype(F32)
        slot = lax.rem(lane, 2).astype(F32)
        tile = lax.rem(lax.div(lane, 2), 8)
        block = meta[yy, column]
        names = jnp.zeros((8, LANES), F32)
        gates = jnp.zeros((8, LANES), F32)
        for k in range(TOP):
            hit = block[:, k : k + 1] == expert
            names = names + jnp.where(hit, 1.0, 0.0)
            gates = gates + jnp.where(hit, block[:, TOP + k : TOP + k + 1], 0.0)
        earlier = shift_rows(names, 1, row)
        for by in (1, 2, 4):
            earlier = earlier + shift_rows(earlier, by, row)
        gates = jnp.where(earlier == slot, gates, 0.0)
        spread = jnp.concatenate([jnp.where(tile == j, gates, 0.0) for j in range(8)], axis=0)
        weights[index] = spread.astype(BF16)

    def square():
        def step(b, carry):
            yy, xx = lax.div(b, NX), lax.rem(b, NX)
            for e in range(4):
                total = jnp.zeros((8, LANES), F32)
                for q in range(chunks):
                    v = raw[q, e, yy, xx].astype(F32)
                    v = v * v
                    total = total + (v[:8] + v[8:])
                squares_of[e, b] = total
            return carry

        lax.fori_loop(0, NX * NY, step, 0)

    def count():
        total_rows = 8 * NX * NY
        blocks = meta[...].reshape(total_rows, LANES)
        column = lax.broadcasted_iota(jnp.int32, (total_rows, LANES), 1)
        odd = lax.rem(lax.broadcasted_iota(jnp.int32, (total_rows, LANES), 0), 2).astype(F32)
        group = lax.div(lax.broadcasted_iota(jnp.int32, (total_rows, total_rows), 0), 8)
        other = lax.div(lax.broadcasted_iota(jnp.int32, (total_rows, total_rows), 1), 8)
        same = jnp.where(group == other, 1.0, 0.0).astype(BF16)
        ones = jnp.ones((LANES, LANES), BF16)
        ids = jnp.where(column < TOP, blocks, -1.0)
        tile = jnp.zeros((8, LANES), F32)
        for e in range(4):
            expert = (me_row * 4 + e).astype(F32)
            hit = jnp.where(ids == expert, 1.0, 0.0).astype(BF16)
            by_token = jnp.dot(hit, ones, preferred_element_type=F32)
            named = jnp.dot(same, by_token.astype(BF16), preferred_element_type=F32)
            squares = squares_of[e].reshape(total_rows, LANES)
            squares = jnp.where(odd < named, squares, 0.0)
            total = jnp.sum(jnp.sum(squares, axis=0, keepdims=True), axis=1, keepdims=True)
            tile = jnp.where(row == e, jnp.broadcast_to(total, (8, LANES)), tile)
            seen = jnp.sum(by_token, axis=0, keepdims=True)
            tile = jnp.where(row == 4 + e, jnp.broadcast_to(seen, (8, LANES)), tile)
        stat[0] = tile
        send(stat.at[0], stat_pair, to_pair, small_sem.at[1], (z, partner))

    def share_stats():
        await_bytes(stat_pair, small_sem.at[1])
        stat[1] = stat[0] + stat_pair[...]
        for k, p in enumerate(z_peers):
            send(stat.at[1], stat_z.at[k], to_z, small_sem.at[2], (p, d))

    def finish_stats():
        await_bytes(stat_z, small_sem.at[2])
        total = stat[1]
        for k in range(NZ - 1):
            total = total + stat_z[k]
        squares = jnp.where(c == 0, total[0:2], total[2:4])
        counts = jnp.where(c == 0, total[4:6], total[6:8])
        stat_ref[0:2] = jnp.sqrt(squares / (counts * float(chunks * 8 * LANES)) + EPS)
        stat_ref[2:4] = counts
        stat_ref[4:8] = jnp.zeros((4, LANES), F32)

    def build_near():
        for h in range(4):
            build(h, h, xr, me_row, y * NX + xl)
            build(4 + h, 4 + h, xl, me_row, y * NX + xr)

    def build_sum():
        for h in range(4):
            build(8 + h, h, x, me_row, y * NX + xr)
            build(12 + h, 4 + h, x, me_row, y * NX + xl)

    def build_ring(step):
        for way in range(2):
            behind = wrap(y + NY - 1 if way == 0 else y + 1, NY) * NX + x
            for xx in range(NX):
                build(16 + 8 * (step - 1) + 4 * way + xx, ring_row(step, way), xx, me_row, behind)

    def build_x_sum():
        for xx in range(NX):
            build(40 + xx, y, xx, me_row, me_row)

    def await_meta():
        await_bytes(meta_rows.at[pl.ds(0, NX * NY - 1)], small_sem.at[0])

    def await_sent():
        await_bytes(x_ref.at[:, :, :, 0], send_sem.at[to_swap])
        for ref, kind in (
            (far_in, to_far), (near_in, to_near), (comb_in, to_comb), (y_in, to_y), (ring_raw, to_ring_raw),
            (ring_in, to_ring), (ring_next, to_ring_next), (ring_half, to_ring_half),
            (via_in, to_via), (x_in, to_x_sum), (meta_rows.at[pl.ds(0, NX * NY - 1)], to_meta),
            (stat_pair, to_pair), (stat_z, to_z),
        ):
            await_bytes(ref, send_sem.at[kind])

    mine, others = 2 * c, 2 - 2 * c
    for q in range(3):
        own_here(q)
        send_far(q, mine, 2)
    for i in range(RING):
        own_here(count_x + i)
        ring_start(i, mine, 2)
    for q in ORDER:
        swap_here(q)
        if q < 3:
            send_far(q, others, 2)
        elif q < count_x:
            own_here(q)
            send_far(q, 0, 4)
        else:
            ring_start(q - count_x, others, 2)
    for i in range(RING):
        ring_more(i)
    send_near(0)
    square()
    await_meta()
    decode()
    build_near()
    send_comb(0)
    build_ring(3)
    for i in range(RING):
        ring_step(i, 3)
    for q in range(1, count_x):
        send_near(q)
        send_comb(q)
    build_ring(2)
    build_sum()
    send_y(0)
    ring_step(0, 2)
    ring_step(1, 2)
    build_ring(1)
    build_x_sum()
    send_y(1)
    pass_on(0)
    ring_step(2, 2)
    count()
    ring_step(0, 1)
    send_y(2)
    share_stats()
    ring_step(1, 1)
    pass_on(1)
    send_y(3)
    ring_step(2, 1)
    pass_on(2)
    send_x_sum(0)
    send_x_sum(1)
    pass_on(3)
    finish_stats()
    finish(0)
    send_x_sum(2)
    finish(1)
    finish_ring(0)
    finish_ring(1)
    finish(2)
    finish_ring(2)
    finish(3)
    await_sent()


def hand_over(in_ref, stat_ref, out_ref, counts_ref, rms_ref):
    out_ref[...] = in_ref[...]
    for e in range(2):
        rms_ref[e] = stat_ref[e, 0]
        counts_ref[e] = stat_ref[2 + e, 0].astype(jnp.int32)


def body(expert_out, expert_ids, gate_weight):
    width = expert_out.shape[4]
    tiles = width // LANES
    chunks = tiles // 8
    view = expert_out.reshape(2, NY, NX, 2, 2, tiles, LANES)
    view = view.transpose(0, 1, 2, 3, 5, 4, 6).reshape(2, NY, NX, 2, tiles * 2, LANES)
    def vmem(*shape):
        return pltpu.VMEM(shape, BF16)

    def dma(*shape):
        return pltpu.SemaphoreType.DMA(shape)

    half = (chunks - RING, 2, 4, 4, ROWS, LANES)
    done = (chunks - RING, 2, 4, TOK, LANES)
    out, stats = pl.pallas_call(
        lambda *refs: kernel(chunks, *refs),
        out_shape=(
            jax.ShapeDtypeStruct((chunks, TOK, LANES), BF16),
            jax.ShapeDtypeStruct((8, LANES), F32),
        ),
        in_specs=[
            pl.BlockSpec(memory_space=pltpu.HBM),
            pl.BlockSpec(memory_space=pltpu.HBM),
            pl.BlockSpec(memory_space=pltpu.HBM),
        ],
        out_specs=(pl.BlockSpec(memory_space=pltpu.VMEM), pl.BlockSpec(memory_space=pltpu.VMEM)),
        scratch_shapes=[
            vmem(chunks, 4, NY, NX, ROWS, LANES),
            vmem(*half), vmem(*half), vmem(*done), vmem(*done),
            vmem(chunks - RING, NY, TOK, LANES), vmem(chunks - RING, 2, TOK + TOK // 2, LANES),
            vmem(chunks - RING, 2, TOK, LANES), vmem(chunks - RING, 2, 2, TOK, LANES),
            vmem(RING, 2, 4, 2, ROWS, LANES), vmem(RING, 2, 4, 2, ROWS, LANES), vmem(RING, 2, 2, TOK, LANES),
            vmem(RING, 3, 2, NX, TOK, LANES), vmem(RING, 2, 2, NX, TOK, LANES),
            vmem(RING, NX, TOK, LANES), vmem(RING, NX - 1, TOK, LANES),
            pltpu.VMEM((TOP, TOP), jnp.int32), pltpu.VMEM((TOP, TOP), F32),
            pltpu.VMEM((NY * NX, 1, LANES), F32), pltpu.VMEM((NY, NX, 8, LANES), F32),
            vmem(44, TOK, LANES), pltpu.VMEM((4, NY * NX, 8, LANES), F32),
            pltpu.VMEM((2, 8, LANES), F32), pltpu.VMEM((8, LANES), F32),
            pltpu.VMEM((NZ - 1, 8, LANES), F32),
            dma(chunks), dma(chunks), dma(chunks - RING), dma(chunks - RING), dma(chunks - RING),
            dma(chunks - RING), dma(chunks - RING), dma(RING, 2), dma(RING, 3), dma(RING), dma(3), dma(14), dma(2),
        ],
        compiler_params=pltpu.CompilerParams(
            collective_id=0, has_side_effects=True, vmem_limit_bytes=54000 * 1024
        ),
    )(view, expert_ids, gate_weight)
    out, counts, rms = pl.pallas_call(
        hand_over,
        out_shape=(
            jax.ShapeDtypeStruct(out.shape, BF16),
            jax.ShapeDtypeStruct((2,), jnp.int32),
            jax.ShapeDtypeStruct((2,), F32),
        ),
        in_specs=[pl.BlockSpec(memory_space=pltpu.VMEM), pl.BlockSpec(memory_space=pltpu.VMEM)],
        out_specs=(
            pl.BlockSpec(memory_space=pltpu.VMEM),
            pl.BlockSpec(memory_space=pltpu.SMEM),
            pl.BlockSpec(memory_space=pltpu.SMEM),
        ),
        compiler_params=pltpu.CompilerParams(vmem_limit_bytes=32 * 1024 * 1024),
    )(out, stats)
    combined = out.reshape(tiles, TOP, LANES).transpose(1, 0, 2).reshape(TOP, width)
    return combined, counts, rms


def solution(mesh):
    return jax.shard_map(
        body,
        mesh=mesh,
        in_specs=(
            P("dp", "expert", None, None, None),
            P(("dp", "expert"), None),
            P(("dp", "expert"), None),
        ),
        out_specs=(P(("dp", "expert"), None), P("expert"), P("expert")),
        check_vma=False,
    )
```
